16 devices in a mesh: dp: 2 (over y, z), ep: 8 (over x, core).
Axes of the slice: x: 4, y: 2, z: 1, core: 2. Of those that a mesh axis runs over, the one named last changes fastest.
The devices are a block of a 4x4x8 slice.
Arguments:
- resid_in: bfloat16 [4096, 2560], P(('dp', 'ep')), parts along dimension 0
- expert_ids: int32 [4096, 6], P(('dp', 'ep')), parts along dimension 0
- priority: int32 [4096, 6], P(('dp', 'ep')), parts along dimension 0
- norm_gain: float32 [2560], replicated
- router_w: bfloat16 [2560, 64], replicated
- shared_w1: bfloat16 [2560, 3072], replicated
- shared_w3: bfloat16 [2560, 3072], replicated
- shared_w2: bfloat16 [3072, 2560], replicated
- expert_w1: bfloat16 [64, 2560, 1536], P('ep')
- expert_w3: bfloat16 [64, 2560, 1536], P('ep')
- expert_w2: bfloat16 [64, 1536, 2560], P('ep')
Outputs:
- output: bfloat16 [4096, 2560], P(('dp', 'ep')), parts along dimension 0
There are 2 independent parts. The reference program is written for one: setup_inputs(seed, part) draws one part's arguments, and reference() takes and returns one part's arrays. A program takes and returns all parts, laid end to end along the dimension named above; an argument that names none is the same for every part.
All inputs are finite; a program needn't handle non-finite values.
Results may differ from the reference program's by a relative error of at most 0.00678837.
Values are sent between devices in bfloat16 or wider.
A program may use at most 768 MiB of HBM per device.

```python
import math
import jax
import jax.numpy as jnp
from jax import lax

HIDDEN = 2560
EXPERTS = 64
TOP_K = 6
EXPERT_FF = 1536
SHARED_FF = 3072
GROUPS = 1
TOP_GROUPS = 1
EP_SIZE = 8
TOKENS = 2048
CAPACITY = 1536

NORM_EPS = 1e-6
ROUTE_SCALE = 16.0


def draw_routing(route_key):
    key_group, key_score, key_hot, key_prio = jax.random.split(route_key, 4)
    group_width = EXPERTS // GROUPS
    n_cand = TOP_GROUPS * group_width
    local_experts = EXPERTS // EP_SIZE
    hot_range = 1280 * TOP_K // n_cand
    hot_dev = jax.random.permutation(key_hot, EP_SIZE) * hot_range // EP_SIZE
    group_score = jax.random.randint(key_group, (TOKENS, GROUPS), 0, 1 << 20) * GROUPS + jnp.arange(GROUPS)
    group_pick = lax.top_k(group_score, TOP_GROUPS)[1]
    cand_ids = (group_pick[:, :, None] * group_width + jnp.arange(group_width)).reshape(TOKENS, n_cand)
    score_noise = jax.random.randint(key_score, (TOKENS, n_cand), 0, 1024)
    cand_score = (score_noise + hot_dev[cand_ids // local_experts]) * n_cand + jnp.arange(n_cand)
    pick_idx = lax.top_k(cand_score, TOP_K)[1]
    expert_ids = jnp.take_along_axis(cand_ids, pick_idx, axis=1).astype(jnp.int32)
    priority = jax.random.permutation(key_prio, TOKENS * TOP_K).reshape(TOKENS, TOP_K).astype(jnp.int32)
    return expert_ids, priority


def setup_inputs(seed: int = 0, part: int = 0) -> dict:
    root_key = jax.random.key(seed)
    resid_key, route_key = jax.random.split(jax.random.fold_in(root_key, part))
    weight_keys = jax.random.split(jax.random.fold_in(root_key, 1 << 30), 8)
    expert_ids, priority = draw_routing(route_key)
    down_gain = EXPERTS / (10.0 * math.sqrt(TOP_K))
    return dict(
        resid_in=jax.random.normal(resid_key, (TOKENS, HIDDEN), jnp.float32).astype(jnp.bfloat16),
        expert_ids=expert_ids,
        priority=priority,
        norm_gain=1.0 + 0.3 * jax.random.normal(weight_keys[0], (HIDDEN,), jnp.float32),
        router_w=(0.5 * HIDDEN ** -0.5 * jax.random.normal(weight_keys[1], (HIDDEN, EXPERTS), jnp.float32)).astype(jnp.bfloat16),
        shared_w1=(HIDDEN ** -0.5 * jax.random.normal(weight_keys[2], (HIDDEN, SHARED_FF), jnp.float32)).astype(jnp.bfloat16),
        shared_w3=(HIDDEN ** -0.5 * jax.random.normal(weight_keys[3], (HIDDEN, SHARED_FF), jnp.float32)).astype(jnp.bfloat16),
        shared_w2=(SHARED_FF ** -0.5 * jax.random.normal(weight_keys[4], (SHARED_FF, HIDDEN), jnp.float32)).astype(jnp.bfloat16),
        expert_w1=(HIDDEN ** -0.5 * jax.random.normal(weight_keys[5], (EXPERTS, HIDDEN, EXPERT_FF), jnp.float32)).astype(jnp.bfloat16),
        expert_w3=(HIDDEN ** -0.5 * jax.random.normal(weight_keys[6], (EXPERTS, HIDDEN, EXPERT_FF), jnp.float32)).astype(jnp.bfloat16),
        expert_w2=(down_gain * EXPERT_FF ** -0.5 * jax.random.normal(weight_keys[7], (EXPERTS, EXPERT_FF, HIDDEN), jnp.float32)).astype(jnp.bfloat16),
    )


def swiglu_ffn(normed, w_gate, w_up, w_down):
    up_a = jnp.dot(normed, w_gate, preferred_element_type=jnp.float32)
    up_b = jnp.dot(normed, w_up, preferred_element_type=jnp.float32)
    hidden_act = (jax.nn.silu(up_a) * up_b).astype(jnp.bfloat16)
    return jnp.dot(hidden_act, w_down, preferred_element_type=jnp.float32).astype(jnp.bfloat16)


def keep_mask(expert_ids, priority):
    n_assign = TOKENS * TOP_K
    owners = (expert_ids // (EXPERTS // EP_SIZE)).reshape(n_assign)
    prio_flat = priority.reshape(n_assign)
    owner_by_rank = jnp.zeros((n_assign,), jnp.int32).at[prio_flat].set(owners)
    dest_hits = (owner_by_rank[:, None] == jnp.arange(EP_SIZE, dtype=jnp.int32)).astype(jnp.int32)
    before = jnp.cumsum(dest_hits, axis=0) - dest_hits
    rank_by_prio = jnp.sum(before * dest_hits, axis=1)
    return (rank_by_prio[prio_flat] < CAPACITY).reshape(TOKENS, TOP_K)


def routed_sum(normed, expert_ids, flat_gates, expert_w1, expert_w3, expert_w2):
    n_assign = TOKENS * TOP_K
    row_block = max(8, n_assign // (32 * EXPERTS) * 8)
    n_blocks = n_assign // row_block + EXPERTS + 1
    flat_ids = expert_ids.reshape(n_assign)
    sort_order = jnp.argsort(flat_ids * n_assign + jnp.arange(n_assign, dtype=jnp.int32)).astype(jnp.int32)
    counts = jax.ops.segment_sum(jnp.ones((n_assign,), jnp.int32), flat_ids, num_segments=EXPERTS)
    padded = (counts + row_block - 1) // row_block * row_block
    pad_start = jnp.cumsum(padded) - padded
    sort_start = jnp.cumsum(counts) - counts
    sorted_ids = flat_ids[sort_order]
    dest_row = pad_start[sorted_ids] + jnp.arange(n_assign, dtype=jnp.int32) - sort_start[sorted_ids]
    row_src = jnp.full((n_blocks * row_block,), n_assign, jnp.int32).at[dest_row].set(sort_order)
    block_first = jnp.arange(n_blocks, dtype=jnp.int32) * row_block
    block_expert = jnp.sum((pad_start[None, :] <= block_first[:, None]).astype(jnp.int32), axis=1) - 1
    normed_pad = jnp.concatenate([normed, jnp.zeros((1, HIDDEN), normed.dtype)], axis=0)
    gates_pad = jnp.concatenate([flat_gates, jnp.zeros((1,), flat_gates.dtype)])

    def one_block(routed_acc, block_args):
        src_rows, expert = block_args
        tok_rows = src_rows // TOP_K
        expert_out = swiglu_ffn(normed_pad[tok_rows], expert_w1[expert], expert_w3[expert], expert_w2[expert])
        weighted = expert_out.astype(jnp.float32) * gates_pad[src_rows][:, None]
        return routed_acc.at[tok_rows].add(weighted), None

    routed_acc = lax.scan(one_block, jnp.zeros((TOKENS + 1, HIDDEN), jnp.float32), (row_src.reshape(n_blocks, row_block), block_expert))[0]
    return routed_acc[:TOKENS]


def reference(resid_in, expert_ids, priority, norm_gain, router_w, shared_w1, shared_w3, shared_w2, expert_w1, expert_w3, expert_w2):
    resid32 = resid_in.astype(jnp.float32)
    inv_rms = lax.rsqrt(jnp.mean(resid32 * resid32, axis=1, keepdims=True) + NORM_EPS)
    normed = (resid32 * inv_rms * norm_gain).astype(jnp.bfloat16)
    gate_probs = jax.nn.softmax(jnp.dot(normed, router_w, preferred_element_type=jnp.float32), axis=1)
    gate_vals = ROUTE_SCALE * jnp.take_along_axis(gate_probs, expert_ids, axis=1)
    kept_mask = keep_mask(expert_ids, priority)
    flat_gates = jnp.where(kept_mask, gate_vals, 0.0).reshape(TOKENS * TOP_K)
    shared_out = swiglu_ffn(normed, shared_w1, shared_w3, shared_w2)
    routed = routed_sum(normed, expert_ids, flat_gates, expert_w1, expert_w3, expert_w2)
    return (resid32 + shared_out.astype(jnp.float32) + routed).astype(jnp.bfloat16)
```

```python
import functools
import jax
import jax.numpy as jnp
from jax import lax
from jax.experimental import pallas as pl
from jax.experimental.pallas import tpu as pltpu
from jax.sharding import PartitionSpec as P

NORM_EPS = 1e-6
ROUTE_SCALE = 16.0
LANES = 128
ROW_TILE = 256
ALIGN = 16
VMEM_LIMIT = 60 * 1024 * 1024
F32, BF16, I32 = jnp.float32, jnp.bfloat16, jnp.int32


def rms_norm(resid_in, norm_gain):
    resid32 = resid_in.astype(F32)
    inv_rms = lax.rsqrt(jnp.mean(resid32 * resid32, axis=1, keepdims=True) + NORM_EPS)
    return (resid32 * inv_rms * norm_gain).astype(BF16)


def gate_values(normed, router_w, expert_ids):
    probs = jax.nn.softmax(jnp.dot(normed, router_w, preferred_element_type=F32), axis=1)
    hit = expert_ids[:, :, None] == jnp.arange(probs.shape[1], dtype=I32)
    return ROUTE_SCALE * jnp.sum(jnp.where(hit, probs[:, None, :], 0.0), axis=2)


def swiglu_ffn(normed, w_gate, w_up, w_down):
    up_a = jnp.dot(normed, w_gate, preferred_element_type=F32)
    up_b = jnp.dot(normed, w_up, preferred_element_type=F32)
    hidden_act = (jax.nn.silu(up_a) * up_b).astype(BF16)
    return jnp.dot(hidden_act, w_down, preferred_element_type=F32).astype(BF16)


def meta_exchange(meta, ep_size):
    chips = ep_size // 2
    moves = [(dc, ds) for ds in range(2) for dc in range(chips) if (dc, ds) != (0, 0)]
    seen_from = {0: 0, 1: 1, chips - 1: 2, 2: 3}

    def kernel(meta_ref, out_ref, send_sem, recv_sem, local_sem):
        me = lax.axis_index('ep')
        chip, core = me // 2, lax.rem(me, 2)

        def peer(dc, ds):
            return 2 * lax.rem(chip + dc, chips) + (core if ds == 0 else 1 - core)

        barrier = pltpu.get_barrier_semaphore()
        for dc, ds in moves:
            pl.semaphore_signal(barrier, inc=1, device_id={'ep': peer(dc, ds)}, device_id_type=pl.DeviceIdType.MESH)
        pl.semaphore_wait(barrier, len(moves))
        own = pltpu.make_async_copy(meta_ref, out_ref.at[0], local_sem)
        own.start()
        copies = []
        for i, (dc, ds) in enumerate(moves):
            slot = 4 * ds + seen_from[dc]
            copy = pltpu.make_async_remote_copy(
                src_ref=meta_ref, dst_ref=out_ref.at[slot], send_sem=send_sem.at[i], recv_sem=recv_sem.at[i],
                device_id={'ep': peer(dc, ds)}, device_id_type=pl.DeviceIdType.MESH)
            copy.start()
            copies.append(copy)
        own.wait()
        for copy in copies:
            copy.wait()

    return pl.pallas_call(
        kernel,
        out_shape=jax.ShapeDtypeStruct((ep_size,) + meta.shape, meta.dtype),
        in_specs=[pl.BlockSpec(memory_space=pltpu.VMEM)],
        out_specs=pl.BlockSpec(memory_space=pltpu.VMEM),
        scratch_shapes=[pltpu.SemaphoreType.DMA((len(moves),)), pltpu.SemaphoreType.DMA((len(moves),)), pltpu.SemaphoreType.DMA],
        compiler_params=pltpu.CompilerParams(collective_id=0, has_side_effects=True),
        name='meta_exchange',
    )(meta)


def routing(meta_all, my_index, local_experts, capacity, slots):
    n_blocks, meta_rows, tok_local = meta_all.shape
    halves = tok_local // LANES
    tok_tiles = n_blocks * halves
    slot_tiles = slots // LANES
    n_rows = tok_tiles * 8

    def kernel(me_ref, meta_ref, sel_ref, tok_ref, gate_ref, off_ref, pos_scr, gates_scr):
        me = me_ref[0]

        def rows(first):
            return jnp.concatenate([meta_ref[b, first:first + 8, h * LANES:(h + 1) * LANES] for b in range(n_blocks) for h in range(halves)], axis=0)

        local_e = rows(0) - (me * local_experts).astype(F32)
        prio = rows(8)
        gates_scr[...] = rows(16)
        mine = (local_e >= 0.0) & (local_e < float(local_experts))
        thresh = jnp.zeros((1, 1), F32)
        bit = 1
        while bit < n_rows * LANES:
            bit *= 2
        while bit >= 1:
            trial = thresh + float(bit)
            count = jnp.sum(jnp.where(mine & (prio < trial), 1.0, 0.0), keepdims=True).reshape(1, 1)
            thresh = jnp.where(count <= float(capacity), trial, thresh)
            bit //= 2
        kept = mine & (prio < thresh)
        row_i = lax.broadcasted_iota(I32, (LANES, LANES), 0)
        col_i = lax.broadcasted_iota(I32, (LANES, LANES), 1)
        upper = jnp.where(row_i < col_i, 1.0, 0.0).astype(BF16)
        lower_r = lax.broadcasted_iota(I32, (n_rows, n_rows), 0)
        lower_c = lax.broadcasted_iota(I32, (n_rows, n_rows), 1)
        lower = jnp.where(lower_c < lower_r, 1.0, 0.0).astype(BF16)
        pos = jnp.full((n_rows, LANES), -1.0, F32)
        start = jnp.zeros((1, 1), F32)
        for e in range(local_experts):
            hit = kept & (local_e == float(e))
            ones = jnp.where(hit, 1.0, 0.0)
            ones16 = ones.astype(BF16)
            in_row = jnp.dot(ones16, upper, preferred_element_type=F32)
            above = jnp.sum(jnp.dot(lower, ones16, preferred_element_type=F32), axis=1, keepdims=True)
            pos = jnp.where(hit, start + in_row + above, pos)
            count = jnp.sum(ones, keepdims=True).reshape(1, 1)
            off_ref[e:e + 1, :] = jnp.broadcast_to(start, (1, LANES)).astype(I32)
            off_ref[local_experts + e:local_experts + e + 1, :] = jnp.broadcast_to(count, (1, LANES)).astype(I32)
            start = start + jnp.floor((count + float(ALIGN - 1)) * (1.0 / ALIGN)) * float(ALIGN)
        pos_scr[...] = pos
        eye = row_i == col_i
        lane = lax.broadcasted_iota(I32, (LANES, LANES), 1).astype(F32)

        def slot_tile(i, carry):
            s_id = (row_i + i * LANES).astype(F32)
            tok = jnp.zeros((LANES, LANES), F32)
            gate = jnp.zeros((LANES, LANES), F32)
            for t in range(tok_tiles):
                any_hit = None
                for k in range(6):
                    r = t * 8 + k
                    eq = pos_scr[r:r + 1, :] == s_id
                    gate = jnp.where(eq, gates_scr[r:r + 1, :], gate)
                    any_hit = eq if any_hit is None else any_hit | eq
                tok = jnp.where(any_hit, lane + float(t * LANES), tok)
                sel_ref[pl.ds(pl.multiple_of(i * LANES, LANES), LANES), t * LANES:(t + 1) * LANES] = jnp.where(any_hit, 1.0, 0.0).astype(BF16)
            tok_col = jnp.sum(tok, axis=1, keepdims=True)
            gate_col = jnp.sum(gate, axis=1, keepdims=True)
            tok_ref[pl.ds(i, 1), :] = jnp.sum(jnp.where(eye, tok_col, 0.0), axis=0, keepdims=True).astype(I32)
            gate_ref[pl.ds(i, 1), :] = jnp.sum(jnp.where(eye, gate_col, 0.0), axis=0, keepdims=True)
            return carry

        lax.fori_loop(0, slot_tiles, slot_tile, 0)

    vmem = pl.BlockSpec(memory_space=pltpu.VMEM)
    return pl.pallas_call(
        kernel,
        out_shape=(
            jax.ShapeDtypeStruct((slots, n_blocks * tok_local), BF16),
            jax.ShapeDtypeStruct((slot_tiles, LANES), I32),
            jax.ShapeDtypeStruct((slot_tiles, LANES), F32),
            jax.ShapeDtypeStruct((2 * local_experts, LANES), I32)),
        in_specs=[pl.BlockSpec(memory_space=pltpu.SMEM), vmem],
        out_specs=(vmem, vmem, vmem, vmem),
        scratch_shapes=[pltpu.VMEM((n_rows, LANES), F32), pltpu.VMEM((n_rows, LANES), F32)],
        compiler_params=pltpu.CompilerParams(vmem_limit_bytes=VMEM_LIMIT),
        cost_estimate=pl.CostEstimate(flops=6 * 10 ** 9, bytes_accessed=slots * 4096, transcendentals=0),
        name='routing',
    )(my_index, meta_all)


def expert_hidden(spans, rows_in, expert_w1, expert_w3):
    slots, width = rows_in.shape
    local_experts, _, ff = expert_w1.shape
    block = ff // 2

    def kernel(span_ref, x_ref, w1_ref, w3_ref, h_ref):
        e = pl.program_id(0)
        n = pl.program_id(1)
        start = span_ref[e]
        count = span_ref[local_experts + e]
        col = pl.multiple_of(n * block, LANES)

        def tile(i, carry):
            at = pl.ds(pl.multiple_of(start + i * ROW_TILE, ALIGN), ROW_TILE)
            x = x_ref[at, :]
            up_a = jnp.dot(x, w1_ref[0], preferred_element_type=F32)
            up_b = jnp.dot(x, w3_ref[0], preferred_element_type=F32)
            h_ref[at, pl.ds(col, block)] = (jax.nn.silu(up_a) * up_b).astype(BF16)
            return carry

        lax.fori_loop(0, (count + ROW_TILE - 1) // ROW_TILE, tile, 0)

    w_spec = pl.BlockSpec((1, width, block), lambda e, n, span: (e, 0, n))
    return pl.pallas_call(
        kernel,
        out_shape=jax.ShapeDtypeStruct((slots, ff), BF16),
        grid_spec=pltpu.PrefetchScalarGridSpec(
            num_scalar_prefetch=1, grid=(local_experts, ff // block),
            in_specs=[pl.BlockSpec((slots, width), lambda e, n, span: (0, 0)), w_spec, w_spec],
            out_specs=pl.BlockSpec((slots, ff), lambda e, n, span: (0, 0))),
        compiler_params=pltpu.CompilerParams(vmem_limit_bytes=VMEM_LIMIT, dimension_semantics=('arbitrary', 'arbitrary')),
        cost_estimate=pl.CostEstimate(flops=4 * 1536 * width * ff, bytes_accessed=2 * expert_w1.size * 2, transcendentals=slots * ff),
        name='expert_hidden',
    )(spans, rows_in, expert_w1, expert_w3)


def expert_combine(spans, slot_tok, slot_gate, hidden, expert_w2, first_col, cols, n_tokens):
    slots, ff = hidden.shape
    local_experts = expert_w2.shape[0]
    groups = cols // LANES

    def kernel(span_ref, tok_ref, gate_ref, h_ref, w2_ref, acc_ref, row_scr):
        e = pl.program_id(0)

        @pl.when(e == 0)
        def _():
            acc_ref[...] = jnp.zeros_like(acc_ref)

        start = span_ref[e]
        count = span_ref[local_experts + e]

        def tile(i, carry):
            base = start + i * ROW_TILE
            h = h_ref[pl.ds(pl.multiple_of(base, ALIGN), ROW_TILE), :]
            out = jnp.dot(h, w2_ref[0], preferred_element_type=F32).astype(BF16).astype(F32)
            for g in range(groups):
                row_scr[pl.ds(g, ROW_TILE, stride=groups), :] = out[:, g * LANES:(g + 1) * LANES]

            def one(r, inner):
                s = base + r
                tok = tok_ref[s // LANES, lax.rem(s, LANES)]
                gate = gate_ref[s // LANES, lax.rem(s, LANES)]
                at = pl.ds(pl.multiple_of(tok * groups, groups), groups)
                acc_ref[at, :] = acc_ref[at, :] + gate * row_scr[pl.ds(pl.multiple_of(r * groups, groups), groups), :]
                return inner

            def eight(q, inner):
                for u in range(8):
                    one(q * 8 + u, 0)
                return inner

            todo = jnp.minimum(count - i * ROW_TILE, ROW_TILE)
            lax.fori_loop(0, (todo + 7) // 8, eight, 0)
            return carry

        lax.fori_loop(0, (count + ROW_TILE - 1) // ROW_TILE, tile, 0)

    block_col = first_col // cols
    smem = pl.BlockSpec(memory_space=pltpu.SMEM)
    return pl.pallas_call(
        kernel,
        out_shape=jax.ShapeDtypeStruct((n_tokens * groups, LANES), F32),
        grid_spec=pltpu.PrefetchScalarGridSpec(
            num_scalar_prefetch=3, grid=(local_experts,),
            in_specs=[pl.BlockSpec((slots, ff), lambda e, *_: (0, 0)),
                      pl.BlockSpec((1, ff, cols), lambda e, *_: (e, 0, block_col))],
            out_specs=pl.BlockSpec((n_tokens * groups, LANES), lambda e, *_: (0, 0)),
            scratch_shapes=[pltpu.VMEM((ROW_TILE * groups, LANES), F32)]),
        compiler_params=pltpu.CompilerParams(vmem_limit_bytes=VMEM_LIMIT, dimension_semantics=('arbitrary',)),
        cost_estimate=pl.CostEstimate(flops=2 * 1536 * ff * cols * 3, bytes_accessed=local_experts * ff * cols * 2, transcendentals=0),
        name='expert_combine',
    )(spans, slot_tok, slot_gate, hidden, expert_w2)


def solution(mesh):
    ep_size = mesh.shape['ep']
    chips = ep_size // 2
    tok_spec = P(('dp', 'ep'))
    expert_spec = P('ep')
    fwd = [(d, (d + 2) % ep_size) for d in range(ep_size)]
    bwd = [(d, (d - 2) % ep_size) for d in range(ep_size)]
    swap = [(d, d ^ 1) for d in range(ep_size)]

    def shift(x, pairs):
        return lax.ppermute(x, 'ep', pairs)

    def gather_rows(part):
        half = part.shape[0] // 2
        before = shift(part, fwd)
        after = shift(part, bwd)
        opp_a = shift(before[:half], fwd)
        opp_b = shift(after[half:], bwd)
        same = jnp.concatenate([part, before, after, opp_a, opp_b], axis=0)
        other = shift(same, swap)
        return jnp.concatenate([same, other], axis=0)

    def reduce_rows(sums):
        n = sums.shape[0] // ep_size
        mid = n // 2
        theirs = shift(sums[chips * n:], swap)
        chip = sums[:chips * n] + theirs
        from_before = shift(chip[3 * n:3 * n + mid], fwd)
        from_after = shift(chip[3 * n + mid:], bwd)
        to_after = jnp.concatenate([chip[2 * n:2 * n + mid] + from_before, chip[2 * n + mid:3 * n]], axis=0)
        to_before = jnp.concatenate([chip[n:n + mid], chip[n + mid:2 * n] + from_after], axis=0)
        return chip[:n] + shift(to_after, fwd) + shift(to_before, bwd)

    def device_fn(resid_in, expert_ids, priority, norm_gain, router_w, shared_w1, shared_w3, shared_w2, expert_w1, expert_w3, expert_w2):
        tok_local, width = resid_in.shape
        top_k = expert_ids.shape[1]
        local_experts = expert_w1.shape[0]
        capacity = tok_local * top_k
        n_tokens = tok_local * ep_size
        slots = -(-(capacity + local_experts * ALIGN + ROW_TILE) // LANES) * LANES
        my_index = lax.axis_index('ep').astype(I32).reshape(1)
        normed = rms_norm(resid_in, norm_gain)
        gates = gate_values(normed, router_w, expert_ids)

        def rows8(x, fill):
            return jnp.pad(x.astype(F32).T, ((0, 8 - top_k), (0, 0)), constant_values=fill)

        meta = jnp.concatenate([rows8(expert_ids, -1.0e6), rows8(priority, 0.0), rows8(gates, 0.0)], axis=0)
        meta_all = meta_exchange(meta, ep_size)
        sel, slot_tok, slot_gate, spans = routing(meta_all, my_index, local_experts, capacity, slots)
        spans = spans[:, 0]

        chunks = 4
        piece = width // chunks
        picked = []
        for c in range(chunks):
            part = gather_rows(normed[:, c * piece:(c + 1) * piece])
            picked.append(jnp.dot(sel, part, preferred_element_type=F32).astype(BF16))
        rows_in = jnp.concatenate(picked, axis=1)
        hidden = expert_hidden(spans, rows_in, expert_w1, expert_w3)
        shared_out = swiglu_ffn(normed, shared_w1, shared_w3, shared_w2)

        routed = []
        for first, cols in ((2048, 512), (0, 1024), (1024, 1024)):
            sums = expert_combine(spans, slot_tok, slot_gate, hidden, expert_w2, first, cols, n_tokens)
            routed.append(reduce_rows(sums).reshape(tok_local, cols))
        routed = jnp.concatenate([routed[1], routed[2], routed[0]], axis=1)
        out_sum = resid_in.astype(F32) + shared_out.astype(F32) + routed
        return out_sum.astype(BF16)

    return jax.shard_map(device_fn, mesh=mesh, in_specs=(tok_spec, tok_spec, tok_spec, P(), P(), P(), P(), P(), expert_spec, expert_spec, expert_spec), out_specs=tok_spec, check_vma=False)
```

```python
import functools
import jax
import jax.numpy as jnp
from jax import lax
from jax.experimental import pallas as pl
from jax.experimental.pallas import tpu as pltpu
from jax.sharding import PartitionSpec as P

NORM_EPS = 1e-6
ROUTE_SCALE = 16.0
LANES = 128
ROW_TILE = 256
ALIGN = 16
VMEM_LIMIT = 60 * 1024 * 1024
F32, BF16, I32 = jnp.float32, jnp.bfloat16, jnp.int32


def rms_norm(resid_in, norm_gain):
    resid32 = resid_in.astype(F32)
    inv_rms = lax.rsqrt(jnp.mean(resid32 * resid32, axis=1, keepdims=True) + NORM_EPS)
    return (resid32 * inv_rms * norm_gain).astype(BF16)


def gate_values(normed, router_w, expert_ids):
    probs = jax.nn.softmax(jnp.dot(normed, router_w, preferred_element_type=F32), axis=1)
    hit = expert_ids[:, :, None] == jnp.arange(probs.shape[1], dtype=I32)
    return ROUTE_SCALE * jnp.sum(jnp.where(hit, probs[:, None, :], 0.0), axis=2)


def meta_exchange(meta, ep_size):
    chips = ep_size // 2
    moves = [(dc, ds) for ds in range(2) for dc in range(chips) if (dc, ds) != (0, 0)]
    seen_from = {0: 0, 1: 1, chips - 1: 2, 2: 3}

    def kernel(meta_ref, out_ref, send_sem, recv_sem, local_sem):
        me = lax.axis_index('ep')
        chip, core = me // 2, lax.rem(me, 2)

        def peer(dc, ds):
            return 2 * lax.rem(chip + dc, chips) + (core if ds == 0 else 1 - core)

        barrier = pltpu.get_barrier_semaphore()
        for dc, ds in moves:
            pl.semaphore_signal(barrier, inc=1, device_id={'ep': peer(dc, ds)}, device_id_type=pl.DeviceIdType.MESH)
        pl.semaphore_wait(barrier, len(moves))
        own = pltpu.make_async_copy(meta_ref, out_ref.at[0], local_sem)
        own.start()
        copies = []
        for i, (dc, ds) in enumerate(moves):
            slot = 4 * ds + seen_from[dc]
            copy = pltpu.make_async_remote_copy(
                src_ref=meta_ref, dst_ref=out_ref.at[slot], send_sem=send_sem.at[i], recv_sem=recv_sem.at[i],
                device_id={'ep': peer(dc, ds)}, device_id_type=pl.DeviceIdType.MESH)
            copy.start()
            copies.append(copy)
        own.wait()
        for copy in copies:
            copy.wait()

    return pl.pallas_call(
        kernel,
        out_shape=jax.ShapeDtypeStruct((ep_size,) + meta.shape, meta.dtype),
        in_specs=[pl.BlockSpec(memory_space=pltpu.VMEM)],
        out_specs=pl.BlockSpec(memory_space=pltpu.VMEM),
        scratch_shapes=[pltpu.SemaphoreType.DMA((len(moves),)), pltpu.SemaphoreType.DMA((len(moves),)), pltpu.SemaphoreType.DMA],
        compiler_params=pltpu.CompilerParams(collective_id=0, has_side_effects=True),
        name='meta_exchange',
    )(meta)


def routing(meta_all, my_index, local_experts, capacity, slots):
    n_blocks, meta_rows, tok_local = meta_all.shape
    halves = tok_local // LANES
    tok_tiles = n_blocks * halves
    slot_tiles = slots // LANES
    n_rows = tok_tiles * 8

    def kernel(me_ref, meta_ref, sel_ref, tok_ref, gate_ref, off_ref, pos_scr, gates_scr):
        me = me_ref[0]

        def rows(first):
            return jnp.concatenate([meta_ref[b, first:first + 8, h * LANES:(h + 1) * LANES] for b in range(n_blocks) for h in range(halves)], axis=0)

        local_e = rows(0) - (me * local_experts).astype(F32)
        prio = rows(8)
        gates_scr[...] = rows(16)
        mine = (local_e >= 0.0) & (local_e < float(local_experts))
        thresh = jnp.zeros((1, 1), F32)
        bit = 1
        while bit < n_rows * LANES:
            bit *= 2
        while bit >= 1:
            trial = thresh + float(bit)
            count = jnp.sum(jnp.where(mine & (prio < trial), 1.0, 0.0), keepdims=True).reshape(1, 1)
            thresh = jnp.where(count <= float(capacity), trial, thresh)
            bit //= 2
        kept = mine & (prio < thresh)
        row_i = lax.broadcasted_iota(I32, (LANES, LANES), 0)
        col_i = lax.broadcasted_iota(I32, (LANES, LANES), 1)
        upper = jnp.where(row_i < col_i, 1.0, 0.0).astype(BF16)
        lower_r = lax.broadcasted_iota(I32, (n_rows, n_rows), 0)
        lower_c = lax.broadcasted_iota(I32, (n_rows, n_rows), 1)
        lower = jnp.where(lower_c < lower_r, 1.0, 0.0).astype(BF16)
        pos = jnp.full((n_rows, LANES), -1.0, F32)
        start = jnp.zeros((1, 1), F32)
        for e in range(local_experts):
            hit = kept & (local_e == float(e))
            ones = jnp.where(hit, 1.0, 0.0)
            ones16 = ones.astype(BF16)
            in_row = jnp.dot(ones16, upper, preferred_element_type=F32)
            above = jnp.sum(jnp.dot(lower, ones16, preferred_element_type=F32), axis=1, keepdims=True)
            pos = jnp.where(hit, start + in_row + above, pos)
            count = jnp.sum(ones, keepdims=True).reshape(1, 1)
            off_ref[e:e + 1, :] = jnp.broadcast_to(start, (1, LANES)).astype(I32)
            off_ref[local_experts + e:local_experts + e + 1, :] = jnp.broadcast_to(count, (1, LANES)).astype(I32)
            start = start + jnp.floor((count + float(ALIGN - 1)) * (1.0 / ALIGN)) * float(ALIGN)
        pos_scr[...] = pos
        eye = row_i == col_i
        lane = lax.broadcasted_iota(I32, (LANES, LANES), 1).astype(F32)

        def slot_tile(i, carry):
            s_id = (row_i + i * LANES).astype(F32)
            tok = jnp.zeros((LANES, LANES), F32)
            gate = jnp.zeros((LANES, LANES), F32)
            for t in range(tok_tiles):
                any_hit = None
                for k in range(6):
                    r = t * 8 + k
                    eq = pos_scr[r:r + 1, :] == s_id
                    gate = jnp.where(eq, gates_scr[r:r + 1, :], gate)
                    any_hit = eq if any_hit is None else any_hit | eq
                tok = jnp.where(any_hit, lane + float(t * LANES + 1), tok)
                sel_ref[pl.ds(pl.multiple_of(i * LANES, LANES), LANES), t * LANES:(t + 1) * LANES] = jnp.where(any_hit, 1.0, 0.0).astype(BF16)
            tok_col = jnp.sum(tok, axis=1, keepdims=True) - 1.0
            tok_col = jnp.where(tok_col < 0.0, float(tok_tiles * LANES), tok_col)
            gate_col = jnp.sum(gate, axis=1, keepdims=True)
            tok_ref[pl.ds(i, 1), :] = jnp.sum(jnp.where(eye, tok_col, 0.0), axis=0, keepdims=True).astype(I32)
            gate_ref[pl.ds(i, 1), :] = jnp.sum(jnp.where(eye, gate_col, 0.0), axis=0, keepdims=True)
            return carry

        lax.fori_loop(0, slot_tiles, slot_tile, 0)

    vmem = pl.BlockSpec(memory_space=pltpu.VMEM)
    return pl.pallas_call(
        kernel,
        out_shape=(
            jax.ShapeDtypeStruct((slots, n_blocks * tok_local), BF16),
            jax.ShapeDtypeStruct((slot_tiles, LANES), I32),
            jax.ShapeDtypeStruct((slot_tiles, LANES), F32),
            jax.ShapeDtypeStruct((2 * local_experts, LANES), I32)),
        in_specs=[pl.BlockSpec(memory_space=pltpu.SMEM), vmem],
        out_specs=(vmem, vmem, vmem, vmem),
        scratch_shapes=[pltpu.VMEM((n_rows, LANES), F32), pltpu.VMEM((n_rows, LANES), F32)],
        compiler_params=pltpu.CompilerParams(vmem_limit_bytes=VMEM_LIMIT),
        cost_estimate=pl.CostEstimate(flops=6 * 10 ** 9, bytes_accessed=slots * 4096, transcendentals=0),
        name='routing',
    )(my_index, meta_all)


def expert_hidden(spans, rows_in, expert_w1, expert_w3):
    slots, width = rows_in.shape
    local_experts, _, ff = expert_w1.shape
    block = ff // 2

    def kernel(span_ref, x_ref, w1_ref, w3_ref, h_ref):
        e = pl.program_id(0)
        n = pl.program_id(1)
        start = span_ref[e]
        count = span_ref[local_experts + e]
        col = pl.multiple_of(n * block, LANES)

        def tile(i, carry):
            at = pl.ds(pl.multiple_of(start + i * ROW_TILE, ALIGN), ROW_TILE)
            x = x_ref[at, :]
            up_a = jnp.dot(x, w1_ref[0], preferred_element_type=F32)
            up_b = jnp.dot(x, w3_ref[0], preferred_element_type=F32)
            h_ref[at, pl.ds(col, block)] = (jax.nn.silu(up_a) * up_b).astype(BF16)
            return carry

        lax.fori_loop(0, (count + ROW_TILE - 1) // ROW_TILE, tile, 0)

    w_spec = pl.BlockSpec((1, width, block), lambda e, n, span: (e, 0, n))
    return pl.pallas_call(
        kernel,
        out_shape=jax.ShapeDtypeStruct((slots, ff), BF16),
        grid_spec=pltpu.PrefetchScalarGridSpec(
            num_scalar_prefetch=1, grid=(local_experts, ff // block),
            in_specs=[pl.BlockSpec((slots, width), lambda e, n, span: (0, 0)), w_spec, w_spec],
            out_specs=pl.BlockSpec((slots, ff), lambda e, n, span: (0, 0))),
        compiler_params=pltpu.CompilerParams(vmem_limit_bytes=VMEM_LIMIT, dimension_semantics=('arbitrary', 'arbitrary')),
        cost_estimate=pl.CostEstimate(flops=4 * 1536 * width * ff, bytes_accessed=2 * expert_w1.size * 2, transcendentals=slots * ff),
        name='expert_hidden',
    )(spans, rows_in, expert_w1, expert_w3)


def expert_combine(spans, slot_tok, slot_gate, hidden, expert_w2, n_tokens):
    slots, ff = hidden.shape
    local_experts, _, width = expert_w2.shape
    cols = width // 2
    groups = cols // LANES
    batch = 8

    def kernel(span_ref, tok_ref, gate_ref, h_ref, w2_ref, acc_ref, row_scr):
        e = pl.program_id(1)

        @pl.when(e == 0)
        def _():
            acc_ref[...] = jnp.zeros_like(acc_ref)

        start = span_ref[e]
        count = span_ref[local_experts + e]

        def tile(i, carry):
            base = start + i * ROW_TILE
            h = h_ref[pl.ds(pl.multiple_of(base, ALIGN), ROW_TILE), :]
            out = jnp.dot(h, w2_ref[0], preferred_element_type=F32).astype(BF16).astype(F32)
            for g in range(groups):
                row_scr[pl.ds(g, ROW_TILE, stride=groups), :] = out[:, g * LANES:(g + 1) * LANES]

            def add_rows(q, inner):
                ats, new = [], []
                for u in range(batch):
                    s = base + q * batch + u
                    at = pl.ds(tok_ref[s] * groups, groups)
                    ats.append(at)
                    new.append(acc_ref[0, at, :] + gate_ref[s] * row_scr[pl.ds((q * batch + u) * groups, groups), :])
                for at, value in zip(ats, new):
                    acc_ref[0, at, :] = value
                return inner

            todo = jnp.minimum(count - i * ROW_TILE, ROW_TILE)
            lax.fori_loop(0, (todo + batch - 1) // batch, add_rows, 0)
            return carry

        lax.fori_loop(0, (count + ROW_TILE - 1) // ROW_TILE, tile, 0)

    acc_rows = (n_tokens + 8) * groups
    return pl.pallas_call(
        kernel,
        out_shape=jax.ShapeDtypeStruct((2, acc_rows, LANES), F32),
        grid_spec=pltpu.PrefetchScalarGridSpec(
            num_scalar_prefetch=3, grid=(2, local_experts),
            in_specs=[pl.BlockSpec((slots, ff), lambda n, e, *_: (0, 0)),
                      pl.BlockSpec((1, ff, cols), lambda n, e, *_: (e, 0, n))],
            out_specs=pl.BlockSpec((1, acc_rows, LANES), lambda n, e, *_: (n, 0, 0)),
            scratch_shapes=[pltpu.VMEM((ROW_TILE * groups, LANES), F32)]),
        compiler_params=pltpu.CompilerParams(vmem_limit_bytes=VMEM_LIMIT, dimension_semantics=('arbitrary', 'arbitrary')),
        cost_estimate=pl.CostEstimate(flops=2 * 1536 * ff * width, bytes_accessed=expert_w2.size * 2, transcendentals=0),
        name='expert_combine',
    )(spans, slot_tok, slot_gate, hidden, expert_w2)


def reduce_and_finish(sums, resid_in, normed, shared_w1, shared_w3, shared_w2, ep_size):
    chips = ep_size // 2
    tok_local, width = resid_in.shape
    ff = shared_w1.shape[1]
    groups = width // 2 // LANES
    pieces = 4
    tok_piece = tok_local // 2
    piece_rows = tok_piece * groups
    up_cols = 512
    n_up = ff // up_cols
    down_cols = 512
    n_down = width // down_cols
    add_step = 128

    def kernel(sums_ref, resid_ref, x_ref, w1_ref, w3_ref, w2_ref, out_ref,
               own, pair, opp, home, up_buf, down_buf, hid, shared,
               load_sem, pair_send, pair_recv, fwd_send, fwd_recv, bwd_send, bwd_recv, up_sem, down_sem):
        me = lax.axis_index('ep')
        chip, core = me // 2, lax.rem(me, 2)
        sibling = 2 * chip + 1 - core
        after = 2 * lax.rem(chip + 1, chips) + core
        before = 2 * lax.rem(chip + chips - 1, chips) + core

        def up_copy(j, slot, which):
            src = w1_ref if which == 0 else w3_ref
            return pltpu.make_async_copy(src.at[:, pl.ds(pl.multiple_of(j * up_cols, LANES), up_cols)], up_buf.at[slot, which], up_sem.at[slot, which])

        def down_copy(j, slot):
            return pltpu.make_async_copy(w2_ref.at[:, pl.ds(pl.multiple_of(j * down_cols, LANES), down_cols)], down_buf.at[slot], down_sem.at[slot])

        barrier = pltpu.get_barrier_semaphore()
        for peer in (sibling, after, before):
            pl.semaphore_signal(barrier, inc=1, device_id={'ep': peer}, device_id_type=pl.DeviceIdType.MESH)
        pl.semaphore_wait(barrier, 3)

        def block_piece(b, q):
            return sums_ref.at[q // 2, pl.ds((b * 2 + q % 2) * piece_rows, piece_rows), :]

        def load(o, q):
            return pltpu.make_async_copy(block_piece(o, q), own.at[o, q], load_sem.at[o, q])

        def to_pair(o, q):
            return pltpu.make_async_remote_copy(
                src_ref=block_piece(chips + o, q), dst_ref=pair.at[o, q], send_sem=pair_send.at[o, q], recv_sem=pair_recv.at[o, q],
                device_id={'ep': sibling}, device_id_type=pl.DeviceIdType.MESH)

        def ring(src, dst, send, recv, i, peer):
            return pltpu.make_async_remote_copy(
                src_ref=src, dst_ref=dst, send_sem=send.at[i], recv_sem=recv.at[i],
                device_id={'ep': peer}, device_id_type=pl.DeviceIdType.MESH)

        order = [(o, q) for o in (3, 2, 1, 0) for q in ((0, 2, 1, 3) if o == 3 else (2, 3, 0, 1) if o == 2 else (0, 1, 2, 3))]
        for o, q in order:
            to_pair(o, q).start()
            load(o, q).start()
        for slot in range(2):
            for which in range(2):
                up_copy(slot, slot, which).start()

        def add(o, q, src):
            def step(i, carry):
                at = pl.ds(pl.multiple_of(i * add_step, add_step), add_step)
                own[o, q, at, :] = own[o, q, at, :] + src[at, :]
                return carry

            lax.fori_loop(0, piece_rows // add_step, step, 0)

        def pair_sum(o, q):
            load(o, q).wait()
            to_pair(o, q).wait_recv()
            add(o, q, pair.at[o, q])

        opp_fwd = [ring(own.at[3, q], opp.at[q], fwd_send, fwd_recv, q, after) for q in (0, 1)]
        opp_bwd = [ring(own.at[3, 2 + q], opp.at[2 + q], bwd_send, bwd_recv, q, before) for q in (0, 1)]
        home_fwd = {q: ring(own.at[2, q], home.at[0, q], fwd_send, fwd_recv, 2 + q, after) for q in range(pieces)}
        home_bwd = {q: ring(own.at[1, q], home.at[1, q], bwd_send, bwd_recv, 2 + q, before) for q in range(pieces)}
        for q in (0, 1):
            pair_sum(3, q)
            pair_sum(3, 2 + q)
            opp_fwd[q].start()
            opp_bwd[q].start()
        for q in (0, 1):
            pair_sum(2, 2 + q)
            pair_sum(1, q)
            home_fwd[2 + q].start()
            home_bwd[q].start()
        for q in (0, 1):
            pair_sum(2, q)
            pair_sum(1, 2 + q)

        def up_step(j, carry):
            slot = lax.rem(j, 2)
            up_copy(j, slot, 0).wait()
            up_copy(j, slot, 1).wait()
            up_a = jnp.dot(x_ref[...], up_buf[slot, 0], preferred_element_type=F32)
            up_b = jnp.dot(x_ref[...], up_buf[slot, 1], preferred_element_type=F32)
            hid[:, pl.ds(pl.multiple_of(j * up_cols, LANES), up_cols)] = (jax.nn.silu(up_a) * up_b).astype(BF16)

            @pl.when(j + 2 < n_up)
            def _():
                up_copy(j + 2, slot, 0).start()
                up_copy(j + 2, slot, 1).start()

            return carry

        for slot in range(2):
            down_copy(slot, slot).start()
        lax.fori_loop(0, n_up, up_step, 0)

        def down_step(j, carry):
            slot = lax.rem(j, 2)
            down_copy(j, slot).wait()
            part = jnp.dot(hid[...], down_buf[slot], preferred_element_type=F32)
            shared[:, pl.ds(pl.multiple_of(j * down_cols, LANES), down_cols)] = part.astype(BF16)

            @pl.when(j + 2 < n_down)
            def _():
                down_copy(j + 2, slot).start()

            return carry

        lax.fori_loop(0, n_down, down_step, 0)

        for q in range(pieces):
            pair_sum(0, q)
        for q in (0, 1):
            opp_fwd[q].wait_recv()
            add(2, q, opp.at[q])
            home_fwd[q].start()
            opp_bwd[q].wait_recv()
            add(1, 2 + q, opp.at[2 + q])
            home_bwd[2 + q].start()
        for q in (0, 2, 1, 3):
            home_fwd[q].wait_recv()
            home_bwd[q].wait_recv()
            add(0, q, home.at[0, q])
            add(0, q, home.at[1, q])
            rows = slice((q % 2) * tok_piece, (q % 2 + 1) * tok_piece)
            for g in range(groups):
                col = (q // 2 * groups + g) * LANES
                routed = own[0, q, pl.ds(g, tok_piece, stride=groups), :]
                total = resid_ref[rows, col:col + LANES].astype(F32) + shared[rows, col:col + LANES].astype(F32) + routed
                out_ref[rows, col:col + LANES] = total.astype(BF16)
        for o, q in order:
            to_pair(o, q).wait_send()
        for copy in opp_fwd + opp_bwd + list(home_fwd.values()) + list(home_bwd.values()):
            copy.wait_send()

    hbm = pl.BlockSpec(memory_space=pl.ANY)
    vmem = pl.BlockSpec(memory_space=pltpu.VMEM)
    dma = pltpu.SemaphoreType.DMA
    return pl.pallas_call(
        kernel,
        out_shape=jax.ShapeDtypeStruct((tok_local, width), BF16),
        in_specs=[hbm, vmem, vmem, hbm, hbm, hbm],
        out_specs=vmem,
        scratch_shapes=[
            pltpu.VMEM((chips, pieces, piece_rows, LANES), F32), pltpu.VMEM((chips, pieces, piece_rows, LANES), F32),
            pltpu.VMEM((pieces, piece_rows, LANES), F32), pltpu.VMEM((2, pieces, piece_rows, LANES), F32),
            pltpu.VMEM((2, 2, width, up_cols), BF16), pltpu.VMEM((2, ff, down_cols), BF16),
            pltpu.VMEM((tok_local, ff), BF16), pltpu.VMEM((tok_local, width), BF16),
            dma((chips, pieces)), dma((chips, pieces)), dma((chips, pieces)), dma((6,)), dma((6,)), dma((6,)), dma((6,)), dma((2, 2)), dma((2,))],
        compiler_params=pltpu.CompilerParams(collective_id=1, has_side_effects=True, vmem_limit_bytes=VMEM_LIMIT),
        cost_estimate=pl.CostEstimate(flops=6 * tok_local * width * ff, bytes_accessed=6 * width * ff, transcendentals=tok_local * ff),
        name='reduce_and_finish',
    )(sums, resid_in, normed, shared_w1, shared_w3, shared_w2)


def solution(mesh):
    ep_size = mesh.shape['ep']
    chips = ep_size // 2
    tok_spec = P(('dp', 'ep'))
    expert_spec = P('ep')
    fwd = [(d, (d + 2) % ep_size) for d in range(ep_size)]
    bwd = [(d, (d - 2) % ep_size) for d in range(ep_size)]
    swap = [(d, d ^ 1) for d in range(ep_size)]

    def shift(x, pairs):
        return lax.ppermute(x, 'ep', pairs)

    def gather_rows(part):
        half = part.shape[0] // 2
        before = shift(part, fwd)
        after = shift(part, bwd)
        opp_a = shift(before[:half], fwd)
        opp_b = shift(after[half:], bwd)
        same = jnp.concatenate([part, before, after, opp_a, opp_b], axis=0)
        other = shift(same, swap)
        return jnp.concatenate([same, other], axis=0)

    def device_fn(resid_in, expert_ids, priority, norm_gain, router_w, shared_w1, shared_w3, shared_w2, expert_w1, expert_w3, expert_w2):
        tok_local, width = resid_in.shape
        top_k = expert_ids.shape[1]
        local_experts = expert_w1.shape[0]
        capacity = tok_local * top_k
        n_tokens = tok_local * ep_size
        slots = -(-(capacity + local_experts * ALIGN + ROW_TILE) // LANES) * LANES
        my_index = lax.axis_index('ep').astype(I32).reshape(1)
        normed = rms_norm(resid_in, norm_gain)
        gates = gate_values(normed, router_w, expert_ids)

        def rows8(x, fill):
            return jnp.pad(x.astype(F32).T, ((0, 8 - top_k), (0, 0)), constant_values=fill)

        meta = jnp.concatenate([rows8(expert_ids, -1.0e6), rows8(priority, 0.0), rows8(gates, 0.0)], axis=0)
        meta_all = meta_exchange(meta, ep_size)
        sel, slot_tok, slot_gate, spans = routing(meta_all, my_index, local_experts, capacity, slots)
        spans = spans[:, 0]

        chunks = 4
        piece = width // chunks
        picked = []
        for c in range(chunks):
            part = gather_rows(normed[:, c * piece:(c + 1) * piece])
            picked.append(jnp.dot(sel, part, preferred_element_type=F32).astype(BF16))
        rows_in = jnp.concatenate(picked, axis=1)
        hidden = expert_hidden(spans, rows_in, expert_w1, expert_w3)
        sums = expert_combine(spans, slot_tok.reshape(-1), slot_gate.reshape(-1), hidden, expert_w2, n_tokens)
        return reduce_and_finish(sums, resid_in, normed, shared_w1, shared_w3, shared_w2, ep_size)

    return jax.shard_map(device_fn, mesh=mesh, in_specs=(tok_spec, tok_spec, tok_spec, P(), P(), P(), P(), P(), expert_spec, expert_spec, expert_spec), out_specs=tok_spec, check_vma=False)
```

```python
import functools
import jax
import jax.numpy as jnp
from jax import lax
from jax.experimental import pallas as pl
from jax.experimental.pallas import tpu as pltpu
from jax.sharding import PartitionSpec as P

NORM_EPS = 1e-6
ROUTE_SCALE = 16.0
LANES = 128
ROW_TILE = 256
ALIGN = 16
VMEM_LIMIT = 60 * 1024 * 1024
F32, BF16, I32 = jnp.float32, jnp.bfloat16, jnp.int32


def rms_norm(resid_in, norm_gain):
    resid32 = resid_in.astype(F32)
    inv_rms = lax.rsqrt(jnp.mean(resid32 * resid32, axis=1, keepdims=True) + NORM_EPS)
    return (resid32 * inv_rms * norm_gain).astype(BF16)


def gate_values(normed, router_w, expert_ids):
    probs = jax.nn.softmax(jnp.dot(normed, router_w, preferred_element_type=F32), axis=1)
    hit = expert_ids[:, :, None] == jnp.arange(probs.shape[1], dtype=I32)
    return ROUTE_SCALE * jnp.sum(jnp.where(hit, probs[:, None, :], 0.0), axis=2)


def dispatch(meta, normed, local_experts, capacity, slots, ep_size):
    meta_rows, tok_local = meta.shape
    width = normed.shape[1]
    chips = ep_size // 2
    n_tokens = ep_size * tok_local
    half = tok_local // 2
    chunks = 5
    piece = width // chunks
    halves = tok_local // LANES
    tok_tiles = ep_size * halves
    n_rows = tok_tiles * 8
    used = capacity + local_experts * ALIGN
    slot_tiles = used // LANES
    sel_step = used // 4
    moves = [(dc, ds) for ds in range(2) for dc in range(chips) if (dc, ds) != (0, 0)]
    seen_from = {0: 0, 1: 1, chips - 1: 2, 2: 3}

    def kernel(meta_ref, x_ref, out_ref, tok_ref, gate_ref, span_ref,
               meta_all, rows_all, sel, picked, pos_scr, gate_rows, aux_scr,
               meta_send, meta_recv, send_sem, recv_sem, out_sem):
        me = lax.axis_index('ep')
        chip, core = me // 2, lax.rem(me, 2)

        def peer(dc, ds):
            return 2 * lax.rem(chip + dc, chips) + (core if ds == 0 else 1 - core)

        sibling, after, before = peer(0, 1), peer(1, 0), peer(chips - 1, 0)

        def remote(src, dst, send, recv, device):
            return pltpu.make_async_remote_copy(src_ref=src, dst_ref=dst, send_sem=send, recv_sem=recv,
                                                device_id={'ep': device}, device_id_type=pl.DeviceIdType.MESH)

        barrier = pltpu.get_barrier_semaphore()
        for dc, ds in moves:
            pl.semaphore_signal(barrier, inc=1, device_id={'ep': peer(dc, ds)}, device_id_type=pl.DeviceIdType.MESH)
        pl.semaphore_wait(barrier, len(moves))

        meta_copies = [remote(meta_ref, meta_all.at[4 * ds + seen_from[dc]], meta_send.at[i], meta_recv.at[i], peer(dc, ds))
                       for i, (dc, ds) in enumerate(moves)]
        for copy in meta_copies:
            copy.start()

        def block(c, b, first=0, count=tok_local):
            return rows_all.at[c, pl.ds(b * tok_local + first, count), :]

        def move(kind, c):
            own = x_ref.at[:, pl.ds(c * piece, piece)]
            src, dst, device = [
                (own, block(c, 1), after),
                (own, block(c, 2), before),
                (own, block(c, 4), sibling),
                (block(c, 1, 0, half), block(c, 3, 0, half), after),
                (block(c, 2, half, half), block(c, 3, half, half), before),
                (block(c, 1), block(c, 5), sibling),
                (block(c, 2), block(c, 6), sibling),
                (block(c, 3, 0, half), block(c, 7, 0, half), sibling),
                (block(c, 3, half, half), block(c, 7, half, half), sibling)][kind]
            return remote(src, dst, send_sem.at[kind, c], recv_sem.at[kind, c], device)

        def send_own(c):
            for kind in (0, 1, 2):
                move(kind, c).start()

        def pass_on(c):
            move(0, c).wait_recv()
            move(3, c).start()
            move(5, c).start()
            move(1, c).wait_recv()
            move(4, c).start()
            move(6, c).start()

        def pass_opposite(c):
            move(3, c).wait_recv()
            move(7, c).start()
            move(4, c).wait_recv()
            move(8, c).start()

        def take_rest(c):
            for kind in (2, 5, 6, 7, 8):
                move(kind, c).wait_recv()

        send_own(0)
        send_own(1)
        meta_all[0] = meta_ref[...]
        for c in range(chunks):
            rows_all[c, 0:tok_local, :] = x_ref[:, c * piece:(c + 1) * piece]
        for copy in meta_copies:
            copy.wait_recv()

        def rows(first):
            return jnp.concatenate([meta_all[b, first:first + 8, h * LANES:(h + 1) * LANES] for b in range(ep_size) for h in range(halves)], axis=0)

        local_e = rows(0) - (me * local_experts).astype(F32)
        prio = rows(8)
        gates = rows(16)
        mine = (local_e >= 0.0) & (local_e < float(local_experts))
        mine_prio = jnp.where(mine, prio, 1.0e9)
        thresh = jnp.zeros((1, 1), F32)
        bit = 1
        while bit < n_rows * LANES:
            bit *= 2
        while bit >= 1:
            trial = thresh + float(bit)
            count = jnp.sum(jnp.where(mine_prio < trial, 1.0, 0.0), keepdims=True).reshape(1, 1)
            thresh = jnp.where(count <= float(capacity), trial, thresh)
            bit //= 2
        kept = mine & (prio < thresh)
        row_i = lax.broadcasted_iota(I32, (LANES, LANES), 0)
        col_i = lax.broadcasted_iota(I32, (LANES, LANES), 1)
        upper = jnp.where(row_i < col_i, 1.0, 0.0).astype(BF16)
        lower_r = lax.broadcasted_iota(I32, (n_rows, n_rows), 0)
        lower_c = lax.broadcasted_iota(I32, (n_rows, n_rows), 1)
        lower = jnp.where(lower_c < lower_r, 1.0, 0.0).astype(BF16)
        span_lane = lax.broadcasted_iota(I32, (1, LANES), 1)
        pos = jnp.full((n_rows, LANES), -1.0, F32)
        start = jnp.zeros((1, 1), F32)
        starts = []
        spans = jnp.zeros((1, LANES), F32)
        for e in range(local_experts):
            hit = kept & (local_e == float(e))
            ones = jnp.where(hit, 1.0, 0.0)
            ones16 = ones.astype(BF16)
            in_row = jnp.dot(ones16, upper, preferred_element_type=F32)
            above = jnp.sum(jnp.dot(lower, ones16, preferred_element_type=F32), axis=1, keepdims=True)
            pos = jnp.where(hit, start + in_row + above, pos)
            count = jnp.sum(ones, keepdims=True).reshape(1, 1)
            starts.append(start)
            spans = jnp.where(span_lane == e, start, spans)
            spans = jnp.where(span_lane == local_experts + e, count, spans)
            start = start + jnp.floor((count + float(ALIGN - 1)) * (1.0 / ALIGN)) * float(ALIGN)
            of_e = jnp.where(hit, gates, 0.0)
            for t in range(tok_tiles):
                gate_rows[e:e + 1, t * LANES:(t + 1) * LANES] = jnp.sum(of_e[t * 8:t * 8 + 8, :], axis=0, keepdims=True)
        pos_scr[...] = pos
        span_ref[...] = spans.astype(I32)

        def build(i, carry):
            s_id = (row_i + i * LANES).astype(F32)
            for t in range(tok_tiles):
                any_hit = None
                for k in range(6):
                    r = t * 8 + k
                    eq = pos_scr[r:r + 1, :] == s_id
                    any_hit = eq if any_hit is None else any_hit | eq
                sel[pl.ds(pl.multiple_of(i * LANES, LANES), LANES), t * LANES:(t + 1) * LANES] = jnp.where(any_hit, 1.0, 0.0).astype(BF16)
            return carry

        pass_on(0)
        send_own(2)
        third = slot_tiles // 3
        lax.fori_loop(0, third, build, 0)
        pass_on(1)
        send_own(3)
        lax.fori_loop(third, 2 * third, build, 0)
        pass_opposite(0)
        lax.fori_loop(2 * third, slot_tiles, build, 0)
        pass_on(2)
        send_own(4)

        g32 = gate_rows[...]
        g_hi = g32.astype(BF16)
        rest = g32 - g_hi.astype(F32)
        g_mid = rest.astype(BF16)
        g_lo = (rest - g_mid.astype(F32)).astype(BF16)
        tok_i = lax.broadcasted_iota(I32, (8, n_tokens), 1)
        kind_i = lax.broadcasted_iota(I32, (8, n_tokens), 0)
        numbers = jnp.where(kind_i == 0, tok_i // ALIGN, jnp.where(kind_i == 1, lax.rem(tok_i, ALIGN), 1)).astype(F32).astype(BF16)
        table = jnp.concatenate([g_hi.astype(F32), g_mid.astype(F32), g_lo.astype(F32), numbers.astype(F32)], axis=0).astype(BF16)
        aux_scr[...] = lax.dot_general(sel[...], table, (((1,), (1,)), ((), ())), preferred_element_type=F32)
        eye = row_i == col_i
        lane32 = lax.broadcasted_iota(I32, (LANES, 32), 1)
        sub32 = lax.broadcasted_iota(I32, (LANES, 32), 0)

        def table_row(i, carry):
            aux = aux_scr[pl.ds(pl.multiple_of(i * LANES, LANES), LANES), :]
            s_id = (sub32 + i * LANES).astype(F32)
            owner = jnp.zeros((LANES, 32), F32)
            for e in range(1, local_experts):
                owner = owner + jnp.where(s_id >= starts[e], 1.0, 0.0)
            is_gate = (lane32 < 24) & (lax.rem(lane32, 8).astype(F32) == owner)
            gate_col = jnp.sum(jnp.where(is_gate, aux, 0.0), axis=1, keepdims=True)
            tok_w = jnp.where(lane32 == 24, float(ALIGN), jnp.where(lane32 == 25, 1.0, 0.0))
            hit_col = jnp.sum(jnp.where(lane32 == 26, aux, 0.0), axis=1, keepdims=True)
            tok_col = jnp.sum(aux * tok_w, axis=1, keepdims=True)
            tok_col = jnp.where(hit_col > 0.5, tok_col, float(n_tokens))
            tok_ref[pl.ds(i, 1), :] = jnp.sum(jnp.where(eye, tok_col, 0.0), axis=0, keepdims=True).astype(I32)
            gate_ref[pl.ds(i, 1), :] = jnp.sum(jnp.where(eye, gate_col, 0.0), axis=0, keepdims=True)
            return carry

        lax.fori_loop(0, slot_tiles, table_row, 0)

        def out_copy(c):
            return pltpu.make_async_copy(picked.at[c % 2], out_ref.at[pl.ds(0, used), pl.ds(c * piece, piece)], out_sem.at[c % 2])

        def pick(c):
            take_rest(c)
            if c >= 2:
                out_copy(c - 2).wait()

            def step(i, carry):
                at = pl.ds(pl.multiple_of(i * sel_step, ALIGN), sel_step)
                picked[c % 2, at, :] = jnp.dot(sel[at, :], rows_all[c], preferred_element_type=F32).astype(BF16)
                return carry

            lax.fori_loop(0, used // sel_step, step, 0)
            out_copy(c).start()

        pass_opposite(1)
        pick(0)
        pass_on(3)
        pass_opposite(2)
        pick(1)
        pass_on(4)
        pass_opposite(3)
        pick(2)
        pass_opposite(4)
        pick(3)
        pick(4)
        out_copy(3).wait()
        out_copy(4).wait()
        for copy in meta_copies:
            copy.wait_send()
        for c in range(chunks):
            for kind in range(9):
                move(kind, c).wait_send()

    vmem = pl.BlockSpec(memory_space=pltpu.VMEM)
    dma = pltpu.SemaphoreType.DMA
    table_rows = -(-slot_tiles // 8) * 8
    return pl.pallas_call(
        kernel,
        out_shape=(
            jax.ShapeDtypeStruct((slots, width), BF16),
            jax.ShapeDtypeStruct((table_rows, LANES), I32),
            jax.ShapeDtypeStruct((table_rows, LANES), F32),
            jax.ShapeDtypeStruct((1, LANES), I32)),
        in_specs=[vmem, vmem],
        out_specs=(pl.BlockSpec(memory_space=pl.ANY), vmem, vmem, vmem),
        scratch_shapes=[
            pltpu.VMEM((ep_size, meta_rows, tok_local), F32), pltpu.VMEM((chunks, n_tokens, piece), BF16),
            pltpu.VMEM((used, n_tokens), BF16), pltpu.VMEM((2, used, piece), BF16),
            pltpu.VMEM((n_rows, LANES), F32), pltpu.VMEM((local_experts, n_tokens), F32), pltpu.VMEM((used, 32), F32),
            dma((len(moves),)), dma((len(moves),)), dma((9, chunks)), dma((9, chunks)), dma((2,))],
        compiler_params=pltpu.CompilerParams(collective_id=0, has_side_effects=True, vmem_limit_bytes=VMEM_LIMIT),
        name='dispatch',
    )(meta, normed)


def expert_hidden(spans, rows_in, expert_w1, expert_w3):
    slots, width = rows_in.shape
    local_experts, _, ff = expert_w1.shape
    block = ff // 2

    def kernel(span_ref, x_ref, w1_ref, w3_ref, h_ref):
        e = pl.program_id(0)
        n = pl.program_id(1)
        start = span_ref[e]
        count = span_ref[local_experts + e]
        col = pl.multiple_of(n * block, LANES)

        def tile(i, carry):
            at = pl.ds(pl.multiple_of(start + i * ROW_TILE, ALIGN), ROW_TILE)
            x = x_ref[at, :]
            up_a = jnp.dot(x, w1_ref[0], preferred_element_type=F32)
            up_b = jnp.dot(x, w3_ref[0], preferred_element_type=F32)
            h_ref[at, pl.ds(col, block)] = (jax.nn.silu(up_a) * up_b).astype(BF16)
            return carry

        lax.fori_loop(0, (count + ROW_TILE - 1) // ROW_TILE, tile, 0)

    w_spec = pl.BlockSpec((1, width, block), lambda e, n, span: (e, 0, n))
    return pl.pallas_call(
        kernel,
        out_shape=jax.ShapeDtypeStruct((slots, ff), BF16),
        grid_spec=pltpu.PrefetchScalarGridSpec(
            num_scalar_prefetch=1, grid=(local_experts, ff // block),
            in_specs=[pl.BlockSpec((slots, width), lambda e, n, span: (0, 0)), w_spec, w_spec],
            out_specs=pl.BlockSpec((slots, ff), lambda e, n, span: (0, 0))),
        compiler_params=pltpu.CompilerParams(vmem_limit_bytes=VMEM_LIMIT, dimension_semantics=('arbitrary', 'arbitrary')),
        cost_estimate=pl.CostEstimate(flops=4 * 1536 * width * ff, bytes_accessed=2 * expert_w1.size * 2, transcendentals=slots * ff),
        name='expert_hidden',
    )(spans, rows_in, expert_w1, expert_w3)


def expert_combine(spans, slot_tok, slot_gate, hidden, expert_w2, n_tokens):
    slots, ff = hidden.shape
    local_experts, _, width = expert_w2.shape
    cols = width // 2
    groups = cols // LANES
    batch = 8

    def kernel(span_ref, tok_ref, gate_ref, h_ref, w2_ref, acc_ref, row_scr):
        e = pl.program_id(1)

        @pl.when(e == 0)
        def _():
            acc_ref[...] = jnp.zeros_like(acc_ref)

        start = span_ref[e]
        count = span_ref[local_experts + e]

        def tile(i, carry):
            base = start + i * ROW_TILE
            h = h_ref[pl.ds(pl.multiple_of(base, ALIGN), ROW_TILE), :]
            out = jnp.dot(h, w2_ref[0], preferred_element_type=F32).astype(BF16).astype(F32)
            for g in range(groups):
                row_scr[pl.ds(g, ROW_TILE, stride=groups), :] = out[:, g * LANES:(g + 1) * LANES]

            def add_rows(q, inner):
                ats, new = [], []
                for u in range(batch):
                    s = base + q * batch + u
                    at = pl.ds(tok_ref[s] * groups, groups)
                    ats.append(at)
                    new.append(acc_ref[0, at, :] + gate_ref[s] * row_scr[pl.ds((q * batch + u) * groups, groups), :])
                for at, value in zip(ats, new):
                    acc_ref[0, at, :] = value
                return inner

            todo = jnp.minimum(count - i * ROW_TILE, ROW_TILE)
            lax.fori_loop(0, (todo + batch - 1) // batch, add_rows, 0)
            return carry

        lax.fori_loop(0, (count + ROW_TILE - 1) // ROW_TILE, tile, 0)

    acc_rows = (n_tokens + 8) * groups
    return pl.pallas_call(
        kernel,
        out_shape=jax.ShapeDtypeStruct((2, acc_rows, LANES), F32),
        grid_spec=pltpu.PrefetchScalarGridSpec(
            num_scalar_prefetch=3, grid=(2, local_experts),
            in_specs=[pl.BlockSpec((slots, ff), lambda n, e, *_: (0, 0)),
                      pl.BlockSpec((1, ff, cols), lambda n, e, *_: (e, 0, n))],
            out_specs=pl.BlockSpec((1, acc_rows, LANES), lambda n, e, *_: (n, 0, 0)),
            scratch_shapes=[pltpu.VMEM((ROW_TILE * groups, LANES), F32)]),
        compiler_params=pltpu.CompilerParams(vmem_limit_bytes=VMEM_LIMIT, dimension_semantics=('arbitrary', 'arbitrary')),
        cost_estimate=pl.CostEstimate(flops=2 * 1536 * ff * width, bytes_accessed=expert_w2.size * 2, transcendentals=0),
        name='expert_combine',
    )(spans, slot_tok, slot_gate, hidden, expert_w2)


def reduce_and_finish(sums, resid_in, normed, shared_w1, shared_w3, shared_w2, ep_size):
    chips = ep_size // 2
    tok_local, width = resid_in.shape
    ff = shared_w1.shape[1]
    groups = width // 2 // LANES
    pieces = 4
    tok_piece = tok_local // 2
    piece_rows = tok_piece * groups
    up_cols = 512
    n_up = ff // up_cols
    down_cols = 512
    n_down = width // down_cols
    add_step = 128

    def kernel(sums_ref, resid_ref, x_ref, w1_ref, w3_ref, w2_ref, out_ref,
               own, pair, opp, home, up_buf, down_buf, hid, shared,
               load_sem, pair_send, pair_recv, fwd_send, fwd_recv, bwd_send, bwd_recv, up_sem, down_sem):
        me = lax.axis_index('ep')
        chip, core = me // 2, lax.rem(me, 2)
        sibling = 2 * chip + 1 - core
        after = 2 * lax.rem(chip + 1, chips) + core
        before = 2 * lax.rem(chip + chips - 1, chips) + core

        def up_copy(j, slot, which):
            src = w1_ref if which == 0 else w3_ref
            return pltpu.make_async_copy(src.at[:, pl.ds(pl.multiple_of(j * up_cols, LANES), up_cols)], up_buf.at[slot, which], up_sem.at[slot, which])

        def down_copy(j, slot):
            return pltpu.make_async_copy(w2_ref.at[:, pl.ds(pl.multiple_of(j * down_cols, LANES), down_cols)], down_buf.at[slot], down_sem.at[slot])

        barrier = pltpu.get_barrier_semaphore()
        for peer in (sibling, after, before):
            pl.semaphore_signal(barrier, inc=1, device_id={'ep': peer}, device_id_type=pl.DeviceIdType.MESH)
        pl.semaphore_wait(barrier, 3)

        def block_piece(b, q):
            return sums_ref.at[q // 2, pl.ds((b * 2 + q % 2) * piece_rows, piece_rows), :]

        def load(o, q):
            return pltpu.make_async_copy(block_piece(o, q), own.at[o, q], load_sem.at[o, q])

        def to_pair(o, q):
            return pltpu.make_async_remote_copy(
                src_ref=block_piece(chips + o, q), dst_ref=pair.at[o, q], send_sem=pair_send.at[o, q], recv_sem=pair_recv.at[o, q],
                device_id={'ep': sibling}, device_id_type=pl.DeviceIdType.MESH)

        def ring(src, dst, send, recv, i, peer):
            return pltpu.make_async_remote_copy(
                src_ref=src, dst_ref=dst, send_sem=send.at[i], recv_sem=recv.at[i],
                device_id={'ep': peer}, device_id_type=pl.DeviceIdType.MESH)

        order = [(o, q) for o in (3, 2, 1, 0) for q in ((0, 2, 1, 3) if o == 3 else (2, 3, 0, 1) if o == 2 else (0, 1, 2, 3))]
        for o, q in order:
            to_pair(o, q).start()
            load(o, q).start()
        for slot in range(2):
            for which in range(2):
                up_copy(slot, slot, which).start()

        def add(o, q, src):
            def step(i, carry):
                at = pl.ds(pl.multiple_of(i * add_step, add_step), add_step)
                own[o, q, at, :] = own[o, q, at, :] + src[at, :]
                return carry

            lax.fori_loop(0, piece_rows // add_step, step, 0)

        def pair_sum(o, q):
            load(o, q).wait()
            to_pair(o, q).wait_recv()
            add(o, q, pair.at[o, q])

        opp_fwd = [ring(own.at[3, q], opp.at[q], fwd_send, fwd_recv, q, after) for q in (0, 1)]
        opp_bwd = [ring(own.at[3, 2 + q], opp.at[2 + q], bwd_send, bwd_recv, q, before) for q in (0, 1)]
        home_fwd = {q: ring(own.at[2, q], home.at[0, q], fwd_send, fwd_recv, 2 + q, after) for q in range(pieces)}
        home_bwd = {q: ring(own.at[1, q], home.at[1, q], bwd_send, bwd_recv, 2 + q, before) for q in range(pieces)}
        for q in (0, 1):
            pair_sum(3, q)
            pair_sum(3, 2 + q)
            opp_fwd[q].start()
            opp_bwd[q].start()
        for q in (0, 1):
            pair_sum(2, 2 + q)
            pair_sum(1, q)
            home_fwd[2 + q].start()
            home_bwd[q].start()
        for q in (0, 1):
            pair_sum(2, q)
            pair_sum(1, 2 + q)

        def up_step(j, carry):
            slot = lax.rem(j, 2)
            up_copy(j, slot, 0).wait()
            up_copy(j, slot, 1).wait()
            up_a = jnp.dot(x_ref[...], up_buf[slot, 0], preferred_element_type=F32)
            up_b = jnp.dot(x_ref[...], up_buf[slot, 1], preferred_element_type=F32)
            hid[:, pl.ds(pl.multiple_of(j * up_cols, LANES), up_cols)] = (jax.nn.silu(up_a) * up_b).astype(BF16)

            @pl.when(j + 2 < n_up)
            def _():
                up_copy(j + 2, slot, 0).start()
                up_copy(j + 2, slot, 1).start()

            return carry

        for slot in range(2):
            down_copy(slot, slot).start()
        lax.fori_loop(0, n_up, up_step, 0)

        def down_step(j, carry):
            slot = lax.rem(j, 2)
            down_copy(j, slot).wait()
            part = jnp.dot(hid[...], down_buf[slot], preferred_element_type=F32)
            shared[:, pl.ds(pl.multiple_of(j * down_cols, LANES), down_cols)] = part.astype(BF16)

            @pl.when(j + 2 < n_down)
            def _():
                down_copy(j + 2, slot).start()

            return carry

        lax.fori_loop(0, n_down, down_step, 0)

        for q in range(pieces):
            pair_sum(0, q)
        for q in (0, 1):
            opp_fwd[q].wait_recv()
            add(2, q, opp.at[q])
            home_fwd[q].start()
            opp_bwd[q].wait_recv()
            add(1, 2 + q, opp.at[2 + q])
            home_bwd[2 + q].start()
        for q in (0, 2, 1, 3):
            home_fwd[q].wait_recv()
            home_bwd[q].wait_recv()
            add(0, q, home.at[0, q])
            add(0, q, home.at[1, q])
            rows = slice((q % 2) * tok_piece, (q % 2 + 1) * tok_piece)
            for g in range(groups):
                col = (q // 2 * groups + g) * LANES
                routed = own[0, q, pl.ds(g, tok_piece, stride=groups), :]
                total = resid_ref[rows, col:col + LANES].astype(F32) + shared[rows, col:col + LANES].astype(F32) + routed
                out_ref[rows, col:col + LANES] = total.astype(BF16)
        for o, q in order:
            to_pair(o, q).wait_send()
        for copy in opp_fwd + opp_bwd + list(home_fwd.values()) + list(home_bwd.values()):
            copy.wait_send()

    hbm = pl.BlockSpec(memory_space=pl.ANY)
    vmem = pl.BlockSpec(memory_space=pltpu.VMEM)
    dma = pltpu.SemaphoreType.DMA
    return pl.pallas_call(
        kernel,
        out_shape=jax.ShapeDtypeStruct((tok_local, width), BF16),
        in_specs=[hbm, vmem, vmem, hbm, hbm, hbm],
        out_specs=vmem,
        scratch_shapes=[
            pltpu.VMEM((chips, pieces, piece_rows, LANES), F32), pltpu.VMEM((chips, pieces, piece_rows, LANES), F32),
            pltpu.VMEM((pieces, piece_rows, LANES), F32), pltpu.VMEM((2, pieces, piece_rows, LANES), F32),
            pltpu.VMEM((2, 2, width, up_cols), BF16), pltpu.VMEM((2, ff, down_cols), BF16),
            pltpu.VMEM((tok_local, ff), BF16), pltpu.VMEM((tok_local, width), BF16),
            dma((chips, pieces)), dma((chips, pieces)), dma((chips, pieces)), dma((6,)), dma((6,)), dma((6,)), dma((6,)), dma((2, 2)), dma((2,))],
        compiler_params=pltpu.CompilerParams(collective_id=1, has_side_effects=True, vmem_limit_bytes=VMEM_LIMIT),
        cost_estimate=pl.CostEstimate(flops=6 * tok_local * width * ff, bytes_accessed=6 * width * ff, transcendentals=tok_local * ff),
        name='reduce_and_finish',
    )(sums, resid_in, normed, shared_w1, shared_w3, shared_w2)


def solution(mesh):
    ep_size = mesh.shape['ep']
    tok_spec = P(('dp', 'ep'))
    expert_spec = P('ep')

    def device_fn(resid_in, expert_ids, priority, norm_gain, router_w, shared_w1, shared_w3, shared_w2, expert_w1, expert_w3, expert_w2):
        tok_local, width = resid_in.shape
        top_k = expert_ids.shape[1]
        local_experts = expert_w1.shape[0]
        capacity = tok_local * top_k
        n_tokens = tok_local * ep_size
        slots = -(-(capacity + local_experts * ALIGN + ROW_TILE) // LANES) * LANES
        normed = rms_norm(resid_in, norm_gain)
        gates = gate_values(normed, router_w, expert_ids)

        def rows8(x, fill):
            return jnp.pad(x.astype(F32).T, ((0, 8 - top_k), (0, 0)), constant_values=fill)

        meta = jnp.concatenate([rows8(expert_ids, -1.0e6), rows8(priority, 0.0), rows8(gates, 0.0)], axis=0)
        rows_in, slot_tok, slot_gate, spans = dispatch(meta, normed, local_experts, capacity, slots, ep_size)
        spans = spans.reshape(-1)
        hidden = expert_hidden(spans, rows_in, expert_w1, expert_w3)
        sums = expert_combine(spans, slot_tok.reshape(-1), slot_gate.reshape(-1), hidden, expert_w2, n_tokens)
        return reduce_and_finish(sums, resid_in, normed, shared_w1, shared_w3, shared_w2, ep_size)

    return jax.shard_map(device_fn, mesh=mesh, in_specs=(tok_spec, tok_spec, tok_spec, P(), P(), P(), P(), P(), expert_spec, expert_spec, expert_spec), out_specs=tok_spec, check_vma=False)
```

```python
import functools
import jax
import jax.numpy as jnp
from jax import lax
from jax.experimental import pallas as pl
from jax.experimental.pallas import tpu as pltpu
from jax.sharding import PartitionSpec as P

NORM_EPS = 1e-6
ROUTE_SCALE = 16.0
LANES = 128
ROW_TILE = 256
ALIGN = 16
VMEM_LIMIT = 60 * 1024 * 1024
F32, BF16, I32 = jnp.float32, jnp.bfloat16, jnp.int32


def rms_norm(resid_in, norm_gain):
    resid32 = resid_in.astype(F32)
    inv_rms = lax.rsqrt(jnp.mean(resid32 * resid32, axis=1, keepdims=True) + NORM_EPS)
    return (resid32 * inv_rms * norm_gain).astype(BF16)


def gate_values(normed, router_w, expert_ids):
    probs = jax.nn.softmax(jnp.dot(normed, router_w, preferred_element_type=F32), axis=1)
    hit = expert_ids[:, :, None] == jnp.arange(probs.shape[1], dtype=I32)
    return ROUTE_SCALE * jnp.sum(jnp.where(hit, probs[:, None, :], 0.0), axis=2)


def dispatch(meta, normed, local_experts, capacity, slots, ep_size):
    meta_rows, tok_local = meta.shape
    width = normed.shape[1]
    chips = ep_size // 2
    n_tokens = ep_size * tok_local
    half = tok_local // 2
    chunks = 5
    piece = width // chunks
    halves = tok_local // LANES
    tok_tiles = ep_size * halves
    n_rows = tok_tiles * 8
    used = capacity + local_experts * ALIGN
    slot_tiles = used // LANES
    sel_step = used // 4
    moves = [(dc, ds) for ds in range(2) for dc in range(chips) if (dc, ds) != (0, 0)]
    seen_from = {0: 0, 1: 1, chips - 1: 2, 2: 3}

    def kernel(meta_ref, x_ref, out_ref, tok_ref, gate_ref, span_ref,
               meta_all, rows_all, sel, picked, pos_scr, gate_rows, aux_scr,
               meta_send, meta_recv, send_sem, recv_sem, out_sem):
        me = lax.axis_index('ep')
        chip, core = me // 2, lax.rem(me, 2)

        def peer(dc, ds):
            return 2 * lax.rem(chip + dc, chips) + (core if ds == 0 else 1 - core)

        sibling, after, before = peer(0, 1), peer(1, 0), peer(chips - 1, 0)

        def remote(src, dst, send, recv, device):
            return pltpu.make_async_remote_copy(src_ref=src, dst_ref=dst, send_sem=send, recv_sem=recv,
                                                device_id={'ep': device}, device_id_type=pl.DeviceIdType.MESH)

        barrier = pltpu.get_barrier_semaphore()
        for dc, ds in moves:
            pl.semaphore_signal(barrier, inc=1, device_id={'ep': peer(dc, ds)}, device_id_type=pl.DeviceIdType.MESH)
        pl.semaphore_wait(barrier, len(moves))

        meta_copies = [remote(meta_ref, meta_all.at[4 * ds + seen_from[dc]], meta_send.at[i], meta_recv.at[i], peer(dc, ds))
                       for i, (dc, ds) in enumerate(moves)]
        for copy in meta_copies:
            copy.start()

        def block(c, b, first=0, count=tok_local):
            return rows_all.at[c, pl.ds(b * tok_local + first, count), :]

        def move(kind, c):
            own = x_ref.at[:, pl.ds(c * piece, piece)]
            src, dst, device = [
                (own, block(c, 1), after),
                (own, block(c, 2), before),
                (own, block(c, 4), sibling),
                (block(c, 1, 0, half), block(c, 3, 0, half), after),
                (block(c, 2, half, half), block(c, 3, half, half), before),
                (block(c, 1), block(c, 5), sibling),
                (block(c, 2), block(c, 6), sibling),
                (block(c, 3, 0, half), block(c, 7, 0, half), sibling),
                (block(c, 3, half, half), block(c, 7, half, half), sibling)][kind]
            return remote(src, dst, send_sem.at[kind, c], recv_sem.at[kind, c], device)

        def send_own(c):
            for kind in (0, 1, 2):
                move(kind, c).start()

        def pass_on(c):
            move(0, c).wait_recv()
            move(3, c).start()
            move(5, c).start()
            move(1, c).wait_recv()
            move(4, c).start()
            move(6, c).start()

        def pass_opposite(c):
            move(3, c).wait_recv()
            move(7, c).start()
            move(4, c).wait_recv()
            move(8, c).start()

        def take_rest(c):
            for kind in (2, 5, 6, 7, 8):
                move(kind, c).wait_recv()

        send_own(0)
        send_own(1)
        meta_all[0] = meta_ref[...]
        for c in range(chunks):
            rows_all[c, 0:tok_local, :] = x_ref[:, c * piece:(c + 1) * piece]
        for copy in meta_copies:
            copy.wait_recv()

        def rows(first):
            return jnp.concatenate([meta_all[b, first:first + 8, h * LANES:(h + 1) * LANES] for b in range(ep_size) for h in range(halves)], axis=0)

        local_e = rows(0) - (me * local_experts).astype(F32)
        prio = rows(8)
        gates = rows(16)
        mine = (local_e >= 0.0) & (local_e < float(local_experts))
        mine_prio = jnp.where(mine, prio, 1.0e9)
        thresh = jnp.zeros((1, 1), F32)
        bit = 1
        while bit < n_rows * LANES:
            bit *= 2
        while bit >= 1:
            trial = thresh + float(bit)
            count = jnp.sum(jnp.where(mine_prio < trial, 1.0, 0.0), keepdims=True).reshape(1, 1)
            thresh = jnp.where(count <= float(capacity), trial, thresh)
            bit //= 2
        kept = mine & (prio < thresh)
        row_i = lax.broadcasted_iota(I32, (LANES, LANES), 0)
        col_i = lax.broadcasted_iota(I32, (LANES, LANES), 1)
        upper = jnp.where(row_i < col_i, 1.0, 0.0).astype(BF16)
        lower_r = lax.broadcasted_iota(I32, (n_rows, n_rows), 0)
        lower_c = lax.broadcasted_iota(I32, (n_rows, n_rows), 1)
        lower = jnp.where(lower_c < lower_r, 1.0, 0.0).astype(BF16)
        span_lane = lax.broadcasted_iota(I32, (1, LANES), 1)
        pos = jnp.full((n_rows, LANES), -1.0, F32)
        start = jnp.zeros((1, 1), F32)
        starts = []
        spans = jnp.zeros((1, LANES), F32)
        for e in range(local_experts):
            hit = kept & (local_e == float(e))
            ones = jnp.where(hit, 1.0, 0.0)
            ones16 = ones.astype(BF16)
            in_row = jnp.dot(ones16, upper, preferred_element_type=F32)
            above = jnp.sum(jnp.dot(lower, ones16, preferred_element_type=F32), axis=1, keepdims=True)
            pos = jnp.where(hit, start + in_row + above, pos)
            count = jnp.sum(ones, keepdims=True).reshape(1, 1)
            starts.append(start)
            spans = jnp.where(span_lane == e, start, spans)
            spans = jnp.where(span_lane == local_experts + e, count, spans)
            start = start + jnp.floor((count + float(ALIGN - 1)) * (1.0 / ALIGN)) * float(ALIGN)
            of_e = jnp.where(hit, gates, 0.0)
            for t in range(tok_tiles):
                gate_rows[e:e + 1, t * LANES:(t + 1) * LANES] = jnp.sum(of_e[t * 8:t * 8 + 8, :], axis=0, keepdims=True)
        pos_scr[...] = pos
        span_ref[...] = spans.astype(I32)

        def build(i, carry):
            s_id = (row_i + i * LANES).astype(F32)
            for t in range(tok_tiles):
                any_hit = None
                for k in range(6):
                    r = t * 8 + k
                    eq = pos_scr[r:r + 1, :] == s_id
                    any_hit = eq if any_hit is None else any_hit | eq
                sel[pl.ds(pl.multiple_of(i * LANES, LANES), LANES), t * LANES:(t + 1) * LANES] = jnp.where(any_hit, 1.0, 0.0).astype(BF16)
            return carry

        pass_on(0)
        send_own(2)
        third = slot_tiles // 3
        lax.fori_loop(0, third, build, 0)
        pass_on(1)
        send_own(3)
        lax.fori_loop(third, 2 * third, build, 0)
        pass_opposite(0)
        lax.fori_loop(2 * third, slot_tiles, build, 0)
        pass_on(2)
        send_own(4)

        g32 = gate_rows[...]
        g_hi = g32.astype(BF16)
        rest = g32 - g_hi.astype(F32)
        g_mid = rest.astype(BF16)
        g_lo = (rest - g_mid.astype(F32)).astype(BF16)
        tok_i = lax.broadcasted_iota(I32, (8, n_tokens), 1)
        kind_i = lax.broadcasted_iota(I32, (8, n_tokens), 0)
        numbers = jnp.where(kind_i == 0, tok_i // ALIGN, jnp.where(kind_i == 1, lax.rem(tok_i, ALIGN), 1)).astype(F32).astype(BF16)
        table = jnp.concatenate([g_hi.astype(F32), g_mid.astype(F32), g_lo.astype(F32), numbers.astype(F32)], axis=0).astype(BF16)
        aux_scr[...] = lax.dot_general(sel[...], table, (((1,), (1,)), ((), ())), preferred_element_type=F32)
        eye = row_i == col_i
        lane32 = lax.broadcasted_iota(I32, (LANES, 32), 1)
        sub32 = lax.broadcasted_iota(I32, (LANES, 32), 0)

        def table_row(i, carry):
            aux = aux_scr[pl.ds(pl.multiple_of(i * LANES, LANES), LANES), :]
            s_id = (sub32 + i * LANES).astype(F32)
            owner = jnp.zeros((LANES, 32), F32)
            for e in range(1, local_experts):
                owner = owner + jnp.where(s_id >= starts[e], 1.0, 0.0)
            is_gate = (lane32 < 24) & (lax.rem(lane32, 8).astype(F32) == owner)
            gate_col = jnp.sum(jnp.where(is_gate, aux, 0.0), axis=1, keepdims=True)
            tok_w = jnp.where(lane32 == 24, float(ALIGN), jnp.where(lane32 == 25, 1.0, 0.0))
            hit_col = jnp.sum(jnp.where(lane32 == 26, aux, 0.0), axis=1, keepdims=True)
            tok_col = jnp.sum(aux * tok_w, axis=1, keepdims=True)
            tok_col = jnp.where(hit_col > 0.5, tok_col, float(n_tokens))
            tok_ref[pl.ds(i, 1), :] = jnp.sum(jnp.where(eye, tok_col, 0.0), axis=0, keepdims=True).astype(I32)
            gate_ref[pl.ds(i, 1), :] = jnp.sum(jnp.where(eye, gate_col, 0.0), axis=0, keepdims=True)
            return carry

        lax.fori_loop(0, slot_tiles, table_row, 0)

        def out_copy(c):
            return pltpu.make_async_copy(picked.at[c % 2], out_ref.at[pl.ds(0, used), pl.ds(c * piece, piece)], out_sem.at[c % 2])

        def pick(c):
            take_rest(c)
            if c >= 2:
                out_copy(c - 2).wait()

            def step(i, carry):
                at = pl.ds(pl.multiple_of(i * sel_step, ALIGN), sel_step)
                picked[c % 2, at, :] = jnp.dot(sel[at, :], rows_all[c], preferred_element_type=F32).astype(BF16)
                return carry

            lax.fori_loop(0, used // sel_step, step, 0)
            out_copy(c).start()

        pass_opposite(1)
        pick(0)
        pass_on(3)
        pass_opposite(2)
        pick(1)
        pass_on(4)
        pass_opposite(3)
        pick(2)
        pass_opposite(4)
        pick(3)
        pick(4)
        out_copy(3).wait()
        out_copy(4).wait()
        for copy in meta_copies:
            copy.wait_send()
        for c in range(chunks):
            for kind in range(9):
                move(kind, c).wait_send()

    vmem = pl.BlockSpec(memory_space=pltpu.VMEM)
    dma = pltpu.SemaphoreType.DMA
    table_rows = -(-slot_tiles // 8) * 8
    return pl.pallas_call(
        kernel,
        out_shape=(
            jax.ShapeDtypeStruct((slots, width), BF16),
            jax.ShapeDtypeStruct((table_rows, LANES), I32),
            jax.ShapeDtypeStruct((table_rows, LANES), F32),
            jax.ShapeDtypeStruct((1, LANES), I32)),
        in_specs=[vmem, vmem],
        out_specs=(pl.BlockSpec(memory_space=pl.ANY), vmem, vmem, vmem),
        scratch_shapes=[
            pltpu.VMEM((ep_size, meta_rows, tok_local), F32), pltpu.VMEM((chunks, n_tokens, piece), BF16),
            pltpu.VMEM((used, n_tokens), BF16), pltpu.VMEM((2, used, piece), BF16),
            pltpu.VMEM((n_rows, LANES), F32), pltpu.VMEM((local_experts, n_tokens), F32), pltpu.VMEM((used, 32), F32),
            dma((len(moves),)), dma((len(moves),)), dma((9, chunks)), dma((9, chunks)), dma((2,))],
        compiler_params=pltpu.CompilerParams(collective_id=0, has_side_effects=True, vmem_limit_bytes=VMEM_LIMIT),
        name='dispatch',
    )(meta, normed)


def experts(spans, slot_tok, slot_gate, rows_in, expert_w1, expert_w3, expert_w2, n_tokens, capacity):
    slots, width = rows_in.shape
    local_experts, _, ff = expert_w1.shape
    groups = width // LANES
    up_cols, n_up = 512, ff // 512
    down_cols, n_down = width // 2, 2
    down_groups = down_cols // LANES
    max_items = local_experts + -(-capacity // ROW_TILE)
    acc_rows = (n_tokens + 8) * groups
    sizes = (128, 160, 192, 224, 256)
    batch = 8

    def kernel(span_ref, tok_ref, gate_ref, x_ref, w1_ref, w3_ref, w2_ref, out_ref,
               acc, row_scr, hid, x_tile, up, down, item_e, item_base, item_count, x_sem, up_sem, down_sem, out_sem):
        def plan(e, n):
            count = span_ref[local_experts + e]

            def one(j, m):
                item_e[m] = e
                item_base[m] = span_ref[e] + j * ROW_TILE
                item_count[m] = jnp.minimum(count - j * ROW_TILE, ROW_TILE)
                return m + 1

            return lax.fori_loop(0, (count + ROW_TILE - 1) // ROW_TILE, one, n)

        n_items = lax.fori_loop(0, local_experts, plan, 0)

        def x_copy(i, slot):
            return pltpu.make_async_copy(x_ref.at[pl.ds(pl.multiple_of(item_base[i], ALIGN), ROW_TILE), :], x_tile.at[slot], x_sem.at[slot])

        def up_copy(i, k, which):
            src = w1_ref if which == 0 else w3_ref
            return pltpu.make_async_copy(src.at[item_e[i], :, pl.ds(k * up_cols, up_cols)], up.at[k, which], up_sem.at[k, which])

        def down_copy(i, k):
            return pltpu.make_async_copy(w2_ref.at[item_e[i], :, pl.ds(k * down_cols, down_cols)], down.at[k], down_sem.at[k])

        @pl.when(n_items > 0)
        def _():
            x_copy(0, 0).start()
            for k in range(n_up):
                up_copy(0, k, 0).start()
                up_copy(0, k, 1).start()
            for k in range(n_down):
                down_copy(0, k).start()

        def zero(i, carry):
            acc[pl.ds(pl.multiple_of(i * groups * 8, 8), groups * 8), :] = jnp.zeros((groups * 8, LANES), F32)
            return carry

        lax.fori_loop(0, acc_rows // (groups * 8), zero, 0)

        def item(i, carry):
            slot = lax.rem(i, 2)
            base = item_base[i]
            count = item_count[i]
            more = i + 1 < n_items
            x_copy(i, slot).wait()

            @pl.when(more)
            def _():
                x_copy(i + 1, 1 - slot).start()

            def sized(body):
                low = 0
                for size in sizes:
                    pl.when((count > low) & (count <= size))(functools.partial(body, size))
                    low = size

            for k in range(n_up):
                up_copy(i, k, 0).wait()
                up_copy(i, k, 1).wait()

                def up_part(size, k=k):
                    x = x_tile[slot, :size, :]
                    up_a = jnp.dot(x, up[k, 0], preferred_element_type=F32)
                    up_b = jnp.dot(x, up[k, 1], preferred_element_type=F32)
                    hid[:size, k * up_cols:(k + 1) * up_cols] = (jax.nn.silu(up_a) * up_b).astype(BF16)

                sized(up_part)

                @pl.when(more)
                def _(k=k):
                    up_copy(i + 1, k, 0).start()
                    up_copy(i + 1, k, 1).start()

            for k in range(n_down):
                down_copy(i, k).wait()

                def down_part(size, k=k):
                    out = jnp.dot(hid[:size, :], down[k], preferred_element_type=F32).astype(BF16).astype(F32)
                    for g in range(down_groups):
                        row_scr[pl.ds(k * down_groups + g, size, stride=groups), :] = out[:, g * LANES:(g + 1) * LANES]

                sized(down_part)

                @pl.when(more)
                def _(k=k):
                    down_copy(i + 1, k).start()

            def add_rows(q, inner):
                ats, new = [], []
                for u in range(batch):
                    s = base + q * batch + u
                    at = pl.ds(tok_ref[s] * groups, groups)
                    ats.append(at)
                    new.append(acc[at, :] + gate_ref[s] * row_scr[pl.ds((q * batch + u) * groups, groups), :])
                for at, value in zip(ats, new):
                    acc[at, :] = value
                return inner

            lax.fori_loop(0, (count + batch - 1) // batch, add_rows, 0)
            return carry

        lax.fori_loop(0, n_items, item, 0)
        out = pltpu.make_async_copy(acc, out_ref, out_sem)
        out.start()
        out.wait()

    hbm = pl.BlockSpec(memory_space=pl.ANY)
    dma = pltpu.SemaphoreType.DMA
    return pl.pallas_call(
        kernel,
        out_shape=jax.ShapeDtypeStruct((acc_rows, LANES), F32),
        grid_spec=pltpu.PrefetchScalarGridSpec(
            num_scalar_prefetch=3, grid=(1,), in_specs=[hbm] * 4, out_specs=hbm,
            scratch_shapes=[
                pltpu.VMEM((acc_rows, LANES), F32), pltpu.VMEM((ROW_TILE * groups, LANES), F32),
                pltpu.VMEM((ROW_TILE, ff), BF16), pltpu.VMEM((2, ROW_TILE, width), BF16),
                pltpu.VMEM((n_up, 2, width, up_cols), BF16), pltpu.VMEM((n_down, ff, down_cols), BF16),
                pltpu.SMEM((max_items,), I32), pltpu.SMEM((max_items,), I32), pltpu.SMEM((max_items,), I32),
                dma((2,)), dma((n_up, 2)), dma((n_down,)), dma]),
        compiler_params=pltpu.CompilerParams(vmem_limit_bytes=VMEM_LIMIT),
        cost_estimate=pl.CostEstimate(flops=6 * capacity * width * ff, bytes_accessed=6 * local_experts * width * ff, transcendentals=capacity * ff),
        name='experts',
    )(spans, slot_tok, slot_gate, rows_in, expert_w1, expert_w3, expert_w2)


def reduce_and_finish(sums, resid_in, normed, shared_w1, shared_w3, shared_w2, ep_size):
    chips = ep_size // 2
    tok_local, width = resid_in.shape
    ff = shared_w1.shape[1]
    groups = width // LANES
    pieces = 4
    tok_piece = tok_local // pieces
    piece_rows = tok_piece * groups
    up_cols = 512
    n_up = ff // up_cols
    down_cols = 512
    n_down = width // down_cols
    add_step = 128

    def kernel(sums_ref, resid_ref, x_ref, w1_ref, w3_ref, w2_ref, out_ref,
               own, pair, opp, home, up_buf, down_buf, hid, shared,
               load_sem, pair_send, pair_recv, fwd_send, fwd_recv, bwd_send, bwd_recv, up_sem, down_sem):
        me = lax.axis_index('ep')
        chip, core = me // 2, lax.rem(me, 2)
        sibling = 2 * chip + 1 - core
        after = 2 * lax.rem(chip + 1, chips) + core
        before = 2 * lax.rem(chip + chips - 1, chips) + core

        def up_copy(j, slot, which):
            src = w1_ref if which == 0 else w3_ref
            return pltpu.make_async_copy(src.at[:, pl.ds(pl.multiple_of(j * up_cols, LANES), up_cols)], up_buf.at[slot, which], up_sem.at[slot, which])

        def down_copy(j, slot):
            return pltpu.make_async_copy(w2_ref.at[:, pl.ds(pl.multiple_of(j * down_cols, LANES), down_cols)], down_buf.at[slot], down_sem.at[slot])

        barrier = pltpu.get_barrier_semaphore()
        for peer in (sibling, after, before):
            pl.semaphore_signal(barrier, inc=1, device_id={'ep': peer}, device_id_type=pl.DeviceIdType.MESH)
        pl.semaphore_wait(barrier, 3)

        def block_piece(b, q):
            return sums_ref.at[pl.ds((b * pieces + q) * piece_rows, piece_rows), :]

        def load(o, q):
            return pltpu.make_async_copy(block_piece(o, q), own.at[o, q], load_sem.at[o, q])

        def to_pair(o, q):
            return pltpu.make_async_remote_copy(
                src_ref=block_piece(chips + o, q), dst_ref=pair.at[o, q], send_sem=pair_send.at[o, q], recv_sem=pair_recv.at[o, q],
                device_id={'ep': sibling}, device_id_type=pl.DeviceIdType.MESH)

        def ring(src, dst, send, recv, i, peer):
            return pltpu.make_async_remote_copy(
                src_ref=src, dst_ref=dst, send_sem=send.at[i], recv_sem=recv.at[i],
                device_id={'ep': peer}, device_id_type=pl.DeviceIdType.MESH)

        order = [(o, q) for o in (3, 2, 1, 0) for q in ((0, 2, 1, 3) if o == 3 else (2, 3, 0, 1) if o == 2 else (0, 1, 2, 3))]
        for o, q in order:
            to_pair(o, q).start()
            load(o, q).start()
        for slot in range(2):
            for which in range(2):
                up_copy(slot, slot, which).start()

        def add(o, q, src):
            def step(i, carry):
                at = pl.ds(pl.multiple_of(i * add_step, add_step), add_step)
                own[o, q, at, :] = own[o, q, at, :] + src[at, :]
                return carry

            lax.fori_loop(0, piece_rows // add_step, step, 0)

        def pair_sum(o, q):
            load(o, q).wait()
            to_pair(o, q).wait_recv()
            add(o, q, pair.at[o, q])

        opp_fwd = [ring(own.at[3, q], opp.at[q], fwd_send, fwd_recv, q, after) for q in (0, 1)]
        opp_bwd = [ring(own.at[3, 2 + q], opp.at[2 + q], bwd_send, bwd_recv, q, before) for q in (0, 1)]
        home_fwd = {q: ring(own.at[2, q], home.at[0, q], fwd_send, fwd_recv, 2 + q, after) for q in range(pieces)}
        home_bwd = {q: ring(own.at[1, q], home.at[1, q], bwd_send, bwd_recv, 2 + q, before) for q in range(pieces)}
        for q in (0, 1):
            pair_sum(3, q)
            pair_sum(3, 2 + q)
            opp_fwd[q].start()
            opp_bwd[q].start()
        for q in (0, 1):
            pair_sum(2, 2 + q)
            pair_sum(1, q)
            home_fwd[2 + q].start()
            home_bwd[q].start()
        for q in (0, 1):
            pair_sum(2, q)
            pair_sum(1, 2 + q)

        def up_step(j, carry):
            slot = lax.rem(j, 2)
            up_copy(j, slot, 0).wait()
            up_copy(j, slot, 1).wait()
            up_a = jnp.dot(x_ref[...], up_buf[slot, 0], preferred_element_type=F32)
            up_b = jnp.dot(x_ref[...], up_buf[slot, 1], preferred_element_type=F32)
            hid[:, pl.ds(pl.multiple_of(j * up_cols, LANES), up_cols)] = (jax.nn.silu(up_a) * up_b).astype(BF16)

            @pl.when(j + 2 < n_up)
            def _():
                up_copy(j + 2, slot, 0).start()
                up_copy(j + 2, slot, 1).start()

            return carry

        for slot in range(2):
            down_copy(slot, slot).start()
        lax.fori_loop(0, n_up, up_step, 0)

        def down_step(j, carry):
            slot = lax.rem(j, 2)
            down_copy(j, slot).wait()
            part = jnp.dot(hid[...], down_buf[slot], preferred_element_type=F32)
            shared[:, pl.ds(pl.multiple_of(j * down_cols, LANES), down_cols)] = part.astype(BF16)

            @pl.when(j + 2 < n_down)
            def _():
                down_copy(j + 2, slot).start()

            return carry

        lax.fori_loop(0, n_down, down_step, 0)

        for q in range(pieces):
            pair_sum(0, q)
        for q in (0, 1):
            opp_fwd[q].wait_recv()
            add(2, q, opp.at[q])
            home_fwd[q].start()
            opp_bwd[q].wait_recv()
            add(1, 2 + q, opp.at[2 + q])
            home_bwd[2 + q].start()
        for q in (0, 2, 1, 3):
            home_fwd[q].wait_recv()
            home_bwd[q].wait_recv()
            add(0, q, home.at[0, q])
            add(0, q, home.at[1, q])
            rows = slice(q * tok_piece, (q + 1) * tok_piece)
            for g in range(groups):
                col = g * LANES
                routed = own[0, q, pl.ds(g, tok_piece, stride=groups), :]
                total = resid_ref[rows, col:col + LANES].astype(F32) + shared[rows, col:col + LANES].astype(F32) + routed
                out_ref[rows, col:col + LANES] = total.astype(BF16)
        for o, q in order:
            to_pair(o, q).wait_send()
        for copy in opp_fwd + opp_bwd + list(home_fwd.values()) + list(home_bwd.values()):
            copy.wait_send()

    hbm = pl.BlockSpec(memory_space=pl.ANY)
    vmem = pl.BlockSpec(memory_space=pltpu.VMEM)
    dma = pltpu.SemaphoreType.DMA
    return pl.pallas_call(
        kernel,
        out_shape=jax.ShapeDtypeStruct((tok_local, width), BF16),
        in_specs=[hbm, vmem, vmem, hbm, hbm, hbm],
        out_specs=vmem,
        scratch_shapes=[
            pltpu.VMEM((chips, pieces, piece_rows, LANES), F32), pltpu.VMEM((chips, pieces, piece_rows, LANES), F32),
            pltpu.VMEM((pieces, piece_rows, LANES), F32), pltpu.VMEM((2, pieces, piece_rows, LANES), F32),
            pltpu.VMEM((2, 2, width, up_cols), BF16), pltpu.VMEM((2, ff, down_cols), BF16),
            pltpu.VMEM((tok_local, ff), BF16), pltpu.VMEM((tok_local, width), BF16),
            dma((chips, pieces)), dma((chips, pieces)), dma((chips, pieces)), dma((6,)), dma((6,)), dma((6,)), dma((6,)), dma((2, 2)), dma((2,))],
        compiler_params=pltpu.CompilerParams(collective_id=1, has_side_effects=True, vmem_limit_bytes=VMEM_LIMIT),
        cost_estimate=pl.CostEstimate(flops=6 * tok_local * width * ff, bytes_accessed=6 * width * ff, transcendentals=tok_local * ff),
        name='reduce_and_finish',
    )(sums, resid_in, normed, shared_w1, shared_w3, shared_w2)


def solution(mesh):
    ep_size = mesh.shape['ep']
    tok_spec = P(('dp', 'ep'))
    expert_spec = P('ep')

    def device_fn(resid_in, expert_ids, priority, norm_gain, router_w, shared_w1, shared_w3, shared_w2, expert_w1, expert_w3, expert_w2):
        tok_local, width = resid_in.shape
        top_k = expert_ids.shape[1]
        local_experts = expert_w1.shape[0]
        capacity = tok_local * top_k
        n_tokens = tok_local * ep_size
        slots = -(-(capacity + local_experts * ALIGN + ROW_TILE) // LANES) * LANES
        normed = rms_norm(resid_in, norm_gain)
        gates = gate_values(normed, router_w, expert_ids)

        def rows8(x, fill):
            return jnp.pad(x.astype(F32).T, ((0, 8 - top_k), (0, 0)), constant_values=fill)

        meta = jnp.concatenate([rows8(expert_ids, -1.0e6), rows8(priority, 0.0), rows8(gates, 0.0)], axis=0)
        rows_in, slot_tok, slot_gate, spans = dispatch(meta, normed, local_experts, capacity, slots, ep_size)
        spans = spans.reshape(-1)
        sums = experts(spans, slot_tok.reshape(-1), slot_gate.reshape(-1), rows_in, expert_w1, expert_w3, expert_w2, n_tokens, capacity)
        return reduce_and_finish(sums, resid_in, normed, shared_w1, shared_w3, shared_w2, ep_size)

    return jax.shard_map(device_fn, mesh=mesh, in_specs=(tok_spec, tok_spec, tok_spec, P(), P(), P(), P(), P(), expert_spec, expert_spec, expert_spec), out_specs=tok_spec, check_vma=False)
```

```python
import functools
import jax
import jax.numpy as jnp
from jax import lax
from jax.experimental import pallas as pl
from jax.experimental.pallas import tpu as pltpu
from jax.sharding import PartitionSpec as P

NORM_EPS = 1e-6
ROUTE_SCALE = 16.0
LANES = 128
ROW_TILE = 256
ALIGN = 16
VMEM_LIMIT = 60 * 1024 * 1024
F32, BF16, I32 = jnp.float32, jnp.bfloat16, jnp.int32


def rms_norm(resid_in, norm_gain):
    resid32 = resid_in.astype(F32)
    inv_rms = lax.rsqrt(jnp.mean(resid32 * resid32, axis=1, keepdims=True) + NORM_EPS)
    return (resid32 * inv_rms * norm_gain).astype(BF16)


def gate_values(normed, router_w, expert_ids):
    probs = jax.nn.softmax(jnp.dot(normed, router_w, preferred_element_type=F32), axis=1)
    hit = expert_ids[:, :, None] == jnp.arange(probs.shape[1], dtype=I32)
    return ROUTE_SCALE * jnp.sum(jnp.where(hit, probs[:, None, :], 0.0), axis=2)


def dispatch(meta, normed, local_experts, capacity, slots, ep_size):
    meta_rows, tok_local = meta.shape
    width = normed.shape[1]
    chips = ep_size // 2
    n_tokens = ep_size * tok_local
    half = tok_local // 2
    chunks = 5
    piece = width // chunks
    halves = tok_local // LANES
    tok_tiles = ep_size * halves
    n_rows = tok_tiles * 8
    used = capacity + local_experts * ALIGN
    slot_tiles = used // LANES
    sel_step = used // 4
    moves = [(dc, ds) for ds in range(2) for dc in range(chips) if (dc, ds) != (0, 0)]
    seen_from = {0: 0, 1: 1, chips - 1: 2, 2: 3}

    def kernel(meta_ref, x_ref, out_ref, tok_ref, gate_ref, span_ref,
               meta_all, rows_all, sel, picked, pos_scr, gate_rows, aux_scr,
               meta_send, meta_recv, send_sem, recv_sem, out_sem):
        me = lax.axis_index('ep')
        chip, core = me // 2, lax.rem(me, 2)

        def peer(dc, ds):
            return 2 * lax.rem(chip + dc, chips) + (core if ds == 0 else 1 - core)

        sibling, after, before = peer(0, 1), peer(1, 0), peer(chips - 1, 0)

        def remote(src, dst, send, recv, device):
            return pltpu.make_async_remote_copy(src_ref=src, dst_ref=dst, send_sem=send, recv_sem=recv,
                                                device_id={'ep': device}, device_id_type=pl.DeviceIdType.MESH)

        barrier = pltpu.get_barrier_semaphore()
        for dc, ds in moves:
            pl.semaphore_signal(barrier, inc=1, device_id={'ep': peer(dc, ds)}, device_id_type=pl.DeviceIdType.MESH)
        pl.semaphore_wait(barrier, len(moves))

        meta_copies = [remote(meta_ref, meta_all.at[4 * ds + seen_from[dc]], meta_send.at[i], meta_recv.at[i], peer(dc, ds))
                       for i, (dc, ds) in enumerate(moves)]
        for copy in meta_copies:
            copy.start()

        def block(c, b, first=0, count=tok_local):
            return rows_all.at[c, pl.ds(b * tok_local + first, count), :]

        def move(kind, c):
            own = x_ref.at[:, pl.ds(c * piece, piece)]
            src, dst, device = [
                (own, block(c, 1), after),
                (own, block(c, 2), before),
                (own, block(c, 4), sibling),
                (block(c, 1, 0, half), block(c, 3, 0, half), after),
                (block(c, 2, half, half), block(c, 3, half, half), before),
                (block(c, 1), block(c, 5), sibling),
                (block(c, 2), block(c, 6), sibling),
                (block(c, 3, 0, half), block(c, 7, 0, half), sibling),
                (block(c, 3, half, half), block(c, 7, half, half), sibling)][kind]
            return remote(src, dst, send_sem.at[kind, c], recv_sem.at[kind, c], device)

        def send_own(c):
            for kind in (0, 1, 2):
                move(kind, c).start()

        def pass_on(c):
            move(0, c).wait_recv()
            move(3, c).start()
            move(5, c).start()
            move(1, c).wait_recv()
            move(4, c).start()
            move(6, c).start()

        def pass_opposite(c):
            move(3, c).wait_recv()
            move(7, c).start()
            move(4, c).wait_recv()
            move(8, c).start()

        def take_rest(c):
            for kind in (2, 5, 6, 7, 8):
                move(kind, c).wait_recv()

        send_own(0)
        send_own(1)
        meta_all[0] = meta_ref[...]
        for c in range(chunks):
            rows_all[c, 0:tok_local, :] = x_ref[:, c * piece:(c + 1) * piece]
        for copy in meta_copies:
            copy.wait_recv()

        def rows(first):
            return jnp.concatenate([meta_all[b, first:first + 8, h * LANES:(h + 1) * LANES] for b in range(ep_size) for h in range(halves)], axis=0)

        local_e = rows(0) - (me * local_experts).astype(F32)
        prio = rows(8)
        gates = rows(16)
        mine = (local_e >= 0.0) & (local_e < float(local_experts))
        mine_prio = jnp.where(mine, prio, 1.0e9)
        thresh = jnp.zeros((1, 1), F32)
        bit = 1
        while bit < n_rows * LANES:
            bit *= 2
        while bit >= 1:
            trial = thresh + float(bit)
            count = jnp.sum(jnp.where(mine_prio < trial, 1.0, 0.0), keepdims=True).reshape(1, 1)
            thresh = jnp.where(count <= float(capacity), trial, thresh)
            bit //= 2
        kept = mine & (prio < thresh)
        row_i = lax.broadcasted_iota(I32, (LANES, LANES), 0)
        col_i = lax.broadcasted_iota(I32, (LANES, LANES), 1)
        upper = jnp.where(row_i < col_i, 1.0, 0.0).astype(BF16)
        lower_r = lax.broadcasted_iota(I32, (n_rows, n_rows), 0)
        lower_c = lax.broadcasted_iota(I32, (n_rows, n_rows), 1)
        lower = jnp.where(lower_c < lower_r, 1.0, 0.0).astype(BF16)
        span_lane = lax.broadcasted_iota(I32, (1, LANES), 1)
        pos = jnp.full((n_rows, LANES), -1.0, F32)
        start = jnp.zeros((1, 1), F32)
        starts = []
        spans = jnp.zeros((1, LANES), F32)
        for e in range(local_experts):
            hit = kept & (local_e == float(e))
            ones = jnp.where(hit, 1.0, 0.0)
            ones16 = ones.astype(BF16)
            in_row = jnp.dot(ones16, upper, preferred_element_type=F32)
            above = jnp.sum(jnp.dot(lower, ones16, preferred_element_type=F32), axis=1, keepdims=True)
            pos = jnp.where(hit, start + in_row + above, pos)
            count = jnp.sum(ones, keepdims=True).reshape(1, 1)
            starts.append(start)
            spans = jnp.where(span_lane == e, start, spans)
            spans = jnp.where(span_lane == local_experts + e, count, spans)
            start = start + jnp.floor((count + float(ALIGN - 1)) * (1.0 / ALIGN)) * float(ALIGN)
            of_e = jnp.where(hit, gates, 0.0)
            for t in range(tok_tiles):
                gate_rows[e:e + 1, t * LANES:(t + 1) * LANES] = jnp.sum(of_e[t * 8:t * 8 + 8, :], axis=0, keepdims=True)
        pos_scr[...] = pos
        span_ref[...] = spans.astype(I32)

        def build(i, carry):
            s_id = (row_i + i * LANES).astype(F32)
            for t in range(tok_tiles):
                any_hit = None
                for k in range(6):
                    r = t * 8 + k
                    eq = pos_scr[r:r + 1, :] == s_id
                    any_hit = eq if any_hit is None else any_hit | eq
                sel[pl.ds(pl.multiple_of(i * LANES, LANES), LANES), t * LANES:(t + 1) * LANES] = jnp.where(any_hit, 1.0, 0.0).astype(BF16)
            return carry

        pass_on(0)
        send_own(2)
        third = slot_tiles // 3
        lax.fori_loop(0, third, build, 0)
        pass_on(1)
        send_own(3)
        lax.fori_loop(third, 2 * third, build, 0)
        pass_opposite(0)
        lax.fori_loop(2 * third, slot_tiles, build, 0)
        pass_on(2)
        send_own(4)

        g32 = gate_rows[...]
        g_hi = g32.astype(BF16)
        rest = g32 - g_hi.astype(F32)
        g_mid = rest.astype(BF16)
        g_lo = (rest - g_mid.astype(F32)).astype(BF16)
        tok_i = lax.broadcasted_iota(I32, (8, n_tokens), 1)
        kind_i = lax.broadcasted_iota(I32, (8, n_tokens), 0)
        numbers = jnp.where(kind_i == 0, tok_i // ALIGN, jnp.where(kind_i == 1, lax.rem(tok_i, ALIGN), 1)).astype(F32).astype(BF16)
        table = jnp.concatenate([g_hi.astype(F32), g_mid.astype(F32), g_lo.astype(F32), numbers.astype(F32)], axis=0).astype(BF16)
        aux_scr[...] = lax.dot_general(sel[...], table, (((1,), (1,)), ((), ())), preferred_element_type=F32)
        eye = row_i == col_i
        lane32 = lax.broadcasted_iota(I32, (LANES, 32), 1)
        sub32 = lax.broadcasted_iota(I32, (LANES, 32), 0)

        def table_row(i, carry):
            aux = aux_scr[pl.ds(pl.multiple_of(i * LANES, LANES), LANES), :]
            s_id = (sub32 + i * LANES).astype(F32)
            owner = jnp.zeros((LANES, 32), F32)
            for e in range(1, local_experts):
                owner = owner + jnp.where(s_id >= starts[e], 1.0, 0.0)
            is_gate = (lane32 < 24) & (lax.rem(lane32, 8).astype(F32) == owner)
            gate_col = jnp.sum(jnp.where(is_gate, aux, 0.0), axis=1, keepdims=True)
            tok_w = jnp.where(lane32 == 24, float(ALIGN), jnp.where(lane32 == 25, 1.0, 0.0))
            hit_col = jnp.sum(jnp.where(lane32 == 26, aux, 0.0), axis=1, keepdims=True)
            tok_col = jnp.sum(aux * tok_w, axis=1, keepdims=True)
            tok_col = jnp.where(hit_col > 0.5, tok_col, float(n_tokens))
            tok_ref[pl.ds(i, 1), :] = jnp.sum(jnp.where(eye, tok_col, 0.0), axis=0, keepdims=True).astype(I32)
            gate_ref[pl.ds(i, 1), :] = jnp.sum(jnp.where(eye, gate_col, 0.0), axis=0, keepdims=True)
            return carry

        lax.fori_loop(0, slot_tiles, table_row, 0)

        def out_copy(c):
            return pltpu.make_async_copy(picked.at[c % 2], out_ref.at[pl.ds(0, used), pl.ds(c * piece, piece)], out_sem.at[c % 2])

        def pick(c):
            take_rest(c)
            if c >= 2:
                out_copy(c - 2).wait()

            def step(i, carry):
                at = pl.ds(pl.multiple_of(i * sel_step, ALIGN), sel_step)
                picked[c % 2, at, :] = jnp.dot(sel[at, :], rows_all[c], preferred_element_type=F32).astype(BF16)
                return carry

            lax.fori_loop(0, used // sel_step, step, 0)
            out_copy(c).start()

        pass_opposite(1)
        pick(0)
        pass_on(3)
        pass_opposite(2)
        pick(1)
        pass_on(4)
        pass_opposite(3)
        pick(2)
        pass_opposite(4)
        pick(3)
        pick(4)
        out_copy(3).wait()
        out_copy(4).wait()
        for copy in meta_copies:
            copy.wait_send()
        for c in range(chunks):
            for kind in range(9):
                move(kind, c).wait_send()

    vmem = pl.BlockSpec(memory_space=pltpu.VMEM)
    dma = pltpu.SemaphoreType.DMA
    table_rows = -(-slot_tiles // 8) * 8
    return pl.pallas_call(
        kernel,
        out_shape=(
            jax.ShapeDtypeStruct((slots, width), BF16),
            jax.ShapeDtypeStruct((table_rows, LANES), I32),
            jax.ShapeDtypeStruct((table_rows, LANES), F32),
            jax.ShapeDtypeStruct((1, LANES), I32)),
        in_specs=[vmem, vmem],
        out_specs=(pl.BlockSpec(memory_space=pl.ANY), vmem, vmem, vmem),
        scratch_shapes=[
            pltpu.VMEM((ep_size, meta_rows, tok_local), F32), pltpu.VMEM((chunks, n_tokens, piece), BF16),
            pltpu.VMEM((used, n_tokens), BF16), pltpu.VMEM((2, used, piece), BF16),
            pltpu.VMEM((n_rows, LANES), F32), pltpu.VMEM((local_experts, n_tokens), F32), pltpu.VMEM((used, 32), F32),
            dma((len(moves),)), dma((len(moves),)), dma((9, chunks)), dma((9, chunks)), dma((2,))],
        compiler_params=pltpu.CompilerParams(collective_id=0, has_side_effects=True, vmem_limit_bytes=VMEM_LIMIT),
        name='dispatch',
    )(meta, normed)


def experts(spans, slot_tok, slot_gate, rows_in, expert_w1, expert_w3, expert_w2, n_tokens, capacity):
    slots, width = rows_in.shape
    local_experts, _, ff = expert_w1.shape
    groups = width // LANES
    up_cols, n_up = 512, ff // 512
    down_cols, n_down = width // 2, 2
    down_groups = down_cols // LANES
    max_items = local_experts + -(-capacity // ROW_TILE)
    acc_rows = (n_tokens + 8) * groups
    sizes = (128, 160, 192, 224, 256)
    batch = 8

    def kernel(span_ref, tok_ref, gate_ref, x_ref, w1_ref, w3_ref, w2_ref, acc,
               row_scr, hid, x_tile, up, down, item_e, item_base, item_count, x_sem, up_sem, down_sem):
        def plan(e, n):
            count = span_ref[local_experts + e]

            def one(j, m):
                item_e[m] = e
                item_base[m] = span_ref[e] + j * ROW_TILE
                item_count[m] = jnp.minimum(count - j * ROW_TILE, ROW_TILE)
                return m + 1

            return lax.fori_loop(0, (count + ROW_TILE - 1) // ROW_TILE, one, n)

        n_items = lax.fori_loop(0, local_experts, plan, 0)

        def x_copy(i, slot):
            return pltpu.make_async_copy(x_ref.at[pl.ds(pl.multiple_of(item_base[i], ALIGN), ROW_TILE), :], x_tile.at[slot], x_sem.at[slot])

        def up_copy(i, k, which):
            src = w1_ref if which == 0 else w3_ref
            return pltpu.make_async_copy(src.at[item_e[i], :, pl.ds(k * up_cols, up_cols)], up.at[k, which], up_sem.at[k, which])

        def down_copy(i, k):
            return pltpu.make_async_copy(w2_ref.at[item_e[i], :, pl.ds(k * down_cols, down_cols)], down.at[k], down_sem.at[k])

        @pl.when(n_items > 0)
        def _():
            x_copy(0, 0).start()
            for k in range(n_up):
                up_copy(0, k, 0).start()
                up_copy(0, k, 1).start()
            for k in range(n_down):
                down_copy(0, k).start()

        def zero(i, carry):
            acc[pl.ds(pl.multiple_of(i * groups * 8, 8), groups * 8), :] = jnp.zeros((groups * 8, LANES), F32)
            return carry

        lax.fori_loop(0, acc_rows // (groups * 8), zero, 0)

        def item(i, carry):
            slot = lax.rem(i, 2)
            base = item_base[i]
            count = item_count[i]
            more = i + 1 < n_items
            x_copy(i, slot).wait()

            @pl.when(more)
            def _():
                x_copy(i + 1, 1 - slot).start()

            def sized(body):
                low = 0
                for size in sizes:
                    pl.when((count > low) & (count <= size))(functools.partial(body, size))
                    low = size

            for k in range(n_up):
                up_copy(i, k, 0).wait()
                up_copy(i, k, 1).wait()

                def up_part(size, k=k):
                    x = x_tile[slot, :size, :]
                    up_a = jnp.dot(x, up[k, 0], preferred_element_type=F32)
                    up_b = jnp.dot(x, up[k, 1], preferred_element_type=F32)
                    hid[:size, k * up_cols:(k + 1) * up_cols] = (jax.nn.silu(up_a) * up_b).astype(BF16)

                sized(up_part)

                @pl.when(more)
                def _(k=k):
                    up_copy(i + 1, k, 0).start()
                    up_copy(i + 1, k, 1).start()

            for k in range(n_down):
                down_copy(i, k).wait()

                def down_part(size, k=k):
                    out = jnp.dot(hid[:size, :], down[k], preferred_element_type=F32).astype(BF16).astype(F32)
                    for g in range(down_groups):
                        row_scr[pl.ds(k * down_groups + g, size, stride=groups), :] = out[:, g * LANES:(g + 1) * LANES]

                sized(down_part)

                @pl.when(more)
                def _(k=k):
                    down_copy(i + 1, k).start()

            def add_rows(q, inner):
                ats, new = [], []
                for u in range(batch):
                    s = base + q * batch + u
                    at = pl.ds(tok_ref[s] * groups, groups)
                    ats.append(at)
                    new.append(acc[at, :] + gate_ref[s] * row_scr[pl.ds((q * batch + u) * groups, groups), :])
                for at, value in zip(ats, new):
                    acc[at, :] = value
                return inner

            lax.fori_loop(0, (count + batch - 1) // batch, add_rows, 0)
            return carry

        lax.fori_loop(0, n_items, item, 0)

    hbm = pl.BlockSpec(memory_space=pl.ANY)
    dma = pltpu.SemaphoreType.DMA
    return pl.pallas_call(
        kernel,
        out_shape=pltpu.VMEM((acc_rows, LANES), F32),
        grid_spec=pltpu.PrefetchScalarGridSpec(
            num_scalar_prefetch=3, grid=(), in_specs=[hbm] * 4, out_specs=pl.BlockSpec(memory_space=pltpu.VMEM),
            scratch_shapes=[
                pltpu.VMEM((ROW_TILE * groups, LANES), F32),
                pltpu.VMEM((ROW_TILE, ff), BF16), pltpu.VMEM((2, ROW_TILE, width), BF16),
                pltpu.VMEM((n_up, 2, width, up_cols), BF16), pltpu.VMEM((n_down, ff, down_cols), BF16),
                pltpu.SMEM((max_items,), I32), pltpu.SMEM((max_items,), I32), pltpu.SMEM((max_items,), I32),
                dma((2,)), dma((n_up, 2)), dma((n_down,))]),
        compiler_params=pltpu.CompilerParams(vmem_limit_bytes=34 * 1024 * 1024),
        cost_estimate=pl.CostEstimate(flops=6 * capacity * width * ff, bytes_accessed=6 * local_experts * width * ff, transcendentals=capacity * ff),
        name='experts',
    )(spans, slot_tok, slot_gate, rows_in, expert_w1, expert_w3, expert_w2)


def reduce_and_finish(sums, resid_in, normed, shared_w1, shared_w3, shared_w2, ep_size):
    chips = ep_size // 2
    tok_local, width = resid_in.shape
    ff = shared_w1.shape[1]
    groups = width // LANES
    pieces = 4
    tok_piece = tok_local // pieces
    piece_rows = tok_piece * groups
    up_cols = 256
    n_up = ff // up_cols
    down_cols = 256
    n_down = width // down_cols
    add_step = 128

    def kernel(sums_ref, resid_ref, x_ref, w1_ref, w3_ref, w2_ref, out_ref,
               pair, opp, home, up_buf, down_buf, hid, shared,
               pair_send, pair_recv, fwd_send, fwd_recv, bwd_send, bwd_recv, up_sem, down_sem):
        me = lax.axis_index('ep')
        chip, core = me // 2, lax.rem(me, 2)
        sibling = 2 * chip + 1 - core
        after = 2 * lax.rem(chip + 1, chips) + core
        before = 2 * lax.rem(chip + chips - 1, chips) + core

        def up_copy(j, slot, which):
            src = w1_ref if which == 0 else w3_ref
            return pltpu.make_async_copy(src.at[:, pl.ds(pl.multiple_of(j * up_cols, LANES), up_cols)], up_buf.at[slot, which], up_sem.at[slot, which])

        def down_copy(j, slot):
            return pltpu.make_async_copy(w2_ref.at[:, pl.ds(pl.multiple_of(j * down_cols, LANES), down_cols)], down_buf.at[slot], down_sem.at[slot])

        barrier = pltpu.get_barrier_semaphore()
        for peer in (sibling, after, before):
            pl.semaphore_signal(barrier, inc=1, device_id={'ep': peer}, device_id_type=pl.DeviceIdType.MESH)
        pl.semaphore_wait(barrier, 3)

        def block_piece(b, q):
            return sums_ref.at[pl.ds((b * pieces + q) * piece_rows, piece_rows), :]

        def to_pair(o, q):
            return pltpu.make_async_remote_copy(
                src_ref=block_piece(chips + o, q), dst_ref=pair.at[o, q], send_sem=pair_send.at[o, q], recv_sem=pair_recv.at[o, q],
                device_id={'ep': sibling}, device_id_type=pl.DeviceIdType.MESH)

        def ring(src, dst, send, recv, i, peer):
            return pltpu.make_async_remote_copy(
                src_ref=src, dst_ref=dst, send_sem=send.at[i], recv_sem=recv.at[i],
                device_id={'ep': peer}, device_id_type=pl.DeviceIdType.MESH)

        order = [(o, q) for o in (3, 2, 1, 0) for q in ((0, 2, 1, 3) if o == 3 else (2, 3, 0, 1) if o == 2 else (0, 1, 2, 3))]
        for o, q in order:
            to_pair(o, q).start()
        for slot in range(2):
            for which in range(2):
                up_copy(slot, slot, which).start()

        def add(o, q, src):
            def step(i, carry):
                at = pl.ds(pl.multiple_of(i * add_step, add_step), add_step)
                pair[o, q, at, :] = pair[o, q, at, :] + src[at, :]
                return carry

            lax.fori_loop(0, piece_rows // add_step, step, 0)

        def pair_sum(o, q):
            to_pair(o, q).wait_recv()
            add(o, q, block_piece(o, q))

        opp_fwd = [ring(pair.at[3, q], opp.at[q], fwd_send, fwd_recv, q, after) for q in (0, 1)]
        opp_bwd = [ring(pair.at[3, 2 + q], opp.at[2 + q], bwd_send, bwd_recv, q, before) for q in (0, 1)]
        home_fwd = {q: ring(pair.at[2, q], home.at[0, q], fwd_send, fwd_recv, 2 + q, after) for q in range(pieces)}
        home_bwd = {q: ring(pair.at[1, q], home.at[1, q], bwd_send, bwd_recv, 2 + q, before) for q in range(pieces)}
        for q in (0, 1):
            pair_sum(3, q)
            pair_sum(3, 2 + q)
            opp_fwd[q].start()
            opp_bwd[q].start()
        for q in (0, 1):
            pair_sum(2, 2 + q)
            pair_sum(1, q)
            home_fwd[2 + q].start()
            home_bwd[q].start()
        for q in (0, 1):
            pair_sum(2, q)
            pair_sum(1, 2 + q)

        def up_step(j, carry):
            slot = lax.rem(j, 2)
            up_copy(j, slot, 0).wait()
            up_copy(j, slot, 1).wait()
            up_a = jnp.dot(x_ref[...], up_buf[slot, 0], preferred_element_type=F32)
            up_b = jnp.dot(x_ref[...], up_buf[slot, 1], preferred_element_type=F32)
            hid[:, pl.ds(pl.multiple_of(j * up_cols, LANES), up_cols)] = (jax.nn.silu(up_a) * up_b).astype(BF16)

            @pl.when(j + 2 < n_up)
            def _():
                up_copy(j + 2, slot, 0).start()
                up_copy(j + 2, slot, 1).start()

            return carry

        for slot in range(2):
            down_copy(slot, slot).start()
        lax.fori_loop(0, n_up, up_step, 0)

        def down_step(j, carry):
            slot = lax.rem(j, 2)
            down_copy(j, slot).wait()
            part = jnp.dot(hid[...], down_buf[slot], preferred_element_type=F32)
            shared[:, pl.ds(pl.multiple_of(j * down_cols, LANES), down_cols)] = part.astype(BF16)

            @pl.when(j + 2 < n_down)
            def _():
                down_copy(j + 2, slot).start()

            return carry

        lax.fori_loop(0, n_down, down_step, 0)

        for q in range(pieces):
            pair_sum(0, q)
        for q in (0, 1):
            opp_fwd[q].wait_recv()
            add(2, q, opp.at[q])
            home_fwd[q].start()
            opp_bwd[q].wait_recv()
            add(1, 2 + q, opp.at[2 + q])
            home_bwd[2 + q].start()
        for q in (0, 2, 1, 3):
            home_fwd[q].wait_recv()
            home_bwd[q].wait_recv()
            add(0, q, home.at[0, q])
            add(0, q, home.at[1, q])
            rows = slice(q * tok_piece, (q + 1) * tok_piece)
            for g in range(groups):
                col = g * LANES
                routed = pair[0, q, pl.ds(g, tok_piece, stride=groups), :]
                total = resid_ref[rows, col:col + LANES].astype(F32) + shared[rows, col:col + LANES].astype(F32) + routed
                out_ref[rows, col:col + LANES] = total.astype(BF16)
        for o, q in order:
            to_pair(o, q).wait_send()
        for copy in opp_fwd + opp_bwd + list(home_fwd.values()) + list(home_bwd.values()):
            copy.wait_send()

    hbm = pl.BlockSpec(memory_space=pl.ANY)
    vmem = pl.BlockSpec(memory_space=pltpu.VMEM)
    dma = pltpu.SemaphoreType.DMA
    return pl.pallas_call(
        kernel,
        out_shape=jax.ShapeDtypeStruct((tok_local, width), BF16),
        in_specs=[vmem, vmem, vmem, hbm, hbm, hbm],
        out_specs=vmem,
        scratch_shapes=[
            pltpu.VMEM((chips, pieces, piece_rows, LANES), F32),
            pltpu.VMEM((pieces, piece_rows, LANES), F32), pltpu.VMEM((2, pieces, piece_rows, LANES), F32),
            pltpu.VMEM((2, 2, width, up_cols), BF16), pltpu.VMEM((2, ff, down_cols), BF16),
            pltpu.VMEM((tok_local, ff), BF16), pltpu.VMEM((tok_local, width), BF16),
            dma((chips, pieces)), dma((chips, pieces)), dma((6,)), dma((6,)), dma((6,)), dma((6,)), dma((2, 2)), dma((2,))],
        compiler_params=pltpu.CompilerParams(collective_id=1, has_side_effects=True, vmem_limit_bytes=37 * 1024 * 1024),
        cost_estimate=pl.CostEstimate(flops=6 * tok_local * width * ff, bytes_accessed=6 * width * ff, transcendentals=tok_local * ff),
        name='reduce_and_finish',
    )(pltpu.with_memory_space_constraint(sums, pltpu.VMEM), resid_in, normed, shared_w1, shared_w3, shared_w2)


def solution(mesh):
    ep_size = mesh.shape['ep']
    tok_spec = P(('dp', 'ep'))
    expert_spec = P('ep')

    def device_fn(resid_in, expert_ids, priority, norm_gain, router_w, shared_w1, shared_w3, shared_w2, expert_w1, expert_w3, expert_w2):
        tok_local, width = resid_in.shape
        top_k = expert_ids.shape[1]
        local_experts = expert_w1.shape[0]
        capacity = tok_local * top_k
        n_tokens = tok_local * ep_size
        slots = -(-(capacity + local_experts * ALIGN + ROW_TILE) // LANES) * LANES
        normed = rms_norm(resid_in, norm_gain)
        gates = gate_values(normed, router_w, expert_ids)

        def rows8(x, fill):
            return jnp.pad(x.astype(F32).T, ((0, 8 - top_k), (0, 0)), constant_values=fill)

        meta = jnp.concatenate([rows8(expert_ids, -1.0e6), rows8(priority, 0.0), rows8(gates, 0.0)], axis=0)
        rows_in, slot_tok, slot_gate, spans = dispatch(meta, normed, local_experts, capacity, slots, ep_size)
        spans = spans.reshape(-1)
        sums = experts(spans, slot_tok.reshape(-1), slot_gate.reshape(-1), rows_in, expert_w1, expert_w3, expert_w2, n_tokens, capacity)
        return reduce_and_finish(sums, resid_in, normed, shared_w1, shared_w3, shared_w2, ep_size)

    return jax.shard_map(device_fn, mesh=mesh, in_specs=(tok_spec, tok_spec, tok_spec, P(), P(), P(), P(), P(), expert_spec, expert_spec, expert_spec), out_specs=tok_spec, check_vma=False)
```

```python
import functools
import jax
import jax.numpy as jnp
from jax import lax
from jax.experimental import pallas as pl
from jax.experimental.pallas import tpu as pltpu
from jax.sharding import PartitionSpec as P

NORM_EPS = 1e-6
ROUTE_SCALE = 16.0
LANES = 128
ROW_TILE = 256
ALIGN = 16
F32, BF16, I32 = jnp.float32, jnp.bfloat16, jnp.int32


def norm_and_gates(resid_in, norm_gain, router_t, ids_t, prio_t):
    tok_local, width = resid_in.shape
    top_k = ids_t.shape[0]
    n_experts = router_t.shape[0]

    def kernel(resid_ref, gain_ref, router_ref, ids_ref, prio_ref, x_ref, meta_ref):
        resid32 = resid_ref[...].astype(F32)
        inv_rms = lax.rsqrt(jnp.mean(resid32 * resid32, axis=1, keepdims=True) + NORM_EPS)
        normed = (resid32 * inv_rms * gain_ref[...]).astype(BF16)
        x_ref[...] = normed
        logits = lax.dot_general(normed, router_ref[...], (((1,), (1,)), ((), ())), preferred_element_type=F32)
        powers = jnp.exp(logits - jnp.max(logits, axis=1, keepdims=True))
        probs = powers / jnp.sum(powers, axis=1, keepdims=True)
        meta_ref[0:8, :] = jnp.full((8, tok_local), -1.0e6, F32)
        meta_ref[8:, :] = jnp.zeros((16, tok_local), F32)
        meta_ref[0:top_k, :] = ids_ref[...].astype(F32)
        meta_ref[8:8 + top_k, :] = prio_ref[...].astype(F32)
        eye = lax.broadcasted_iota(I32, (LANES, LANES), 0) == lax.broadcasted_iota(I32, (LANES, LANES), 1)
        expert = lax.broadcasted_iota(I32, (LANES, n_experts), 1).astype(F32)
        for h in range(tok_local // LANES):
            span = slice(h * LANES, (h + 1) * LANES)
            for k in range(top_k):
                id_col = jnp.sum(jnp.where(eye, ids_ref[k:k + 1, span].astype(F32), 0.0), axis=1, keepdims=True)
                gate_col = ROUTE_SCALE * jnp.sum(jnp.where(expert == id_col, probs[span, :], 0.0), axis=1, keepdims=True)
                meta_ref[16 + k:17 + k, span] = jnp.sum(jnp.where(eye, gate_col, 0.0), axis=0, keepdims=True)

    vmem = pl.BlockSpec(memory_space=pltpu.VMEM)
    return pl.pallas_call(
        kernel,
        out_shape=(jax.ShapeDtypeStruct((tok_local, width), BF16), jax.ShapeDtypeStruct((24, tok_local), F32)),
        in_specs=[vmem] * 5, out_specs=(vmem, vmem),
        compiler_params=pltpu.CompilerParams(vmem_limit_bytes=30 * 1024 * 1024),
        name='norm_and_gates',
    )(resid_in, norm_gain.reshape(1, width), router_t, ids_t, prio_t)


def dispatch(meta, normed, local_experts, capacity, slots, ep_size):
    meta_rows, tok_local = meta.shape
    width = normed.shape[1]
    chips = ep_size // 2
    n_tokens = ep_size * tok_local
    half = tok_local // 2
    chunks = 5
    piece = width // chunks
    halves = tok_local // LANES
    tok_tiles = ep_size * halves
    n_rows = tok_tiles * 8
    used = capacity + local_experts * ALIGN
    slot_tiles = used // LANES
    sel_step = used // 2
    moves = [(dc, ds) for ds in range(2) for dc in range(chips) if (dc, ds) != (0, 0)]
    seen_from = {0: 0, 1: 1, chips - 1: 2, 2: 3}

    def kernel(meta_ref, x_ref, out_ref, tok_ref, gate_ref, span_ref,
               meta_all, rows_all, sel, picked, pos_scr, gate_rows, aux_scr,
               meta_send, meta_recv, send_sem, recv_sem, out_sem):
        me = lax.axis_index('ep')
        chip, core = me // 2, lax.rem(me, 2)

        def peer(dc, ds):
            return 2 * lax.rem(chip + dc, chips) + (core if ds == 0 else 1 - core)

        sibling, after, before = peer(0, 1), peer(1, 0), peer(chips - 1, 0)

        def remote(src, dst, send, recv, device):
            return pltpu.make_async_remote_copy(src_ref=src, dst_ref=dst, send_sem=send, recv_sem=recv,
                                                device_id={'ep': device}, device_id_type=pl.DeviceIdType.MESH)

        barrier = pltpu.get_barrier_semaphore()
        for dc, ds in moves:
            pl.semaphore_signal(barrier, inc=1, device_id={'ep': peer(dc, ds)}, device_id_type=pl.DeviceIdType.MESH)
        pl.semaphore_wait(barrier, len(moves))

        meta_copies = [remote(meta_ref, meta_all.at[4 * ds + seen_from[dc]], meta_send.at[i], meta_recv.at[i], peer(dc, ds))
                       for i, (dc, ds) in enumerate(moves)]
        for copy in meta_copies:
            copy.start()

        def block(c, b, first=0, count=tok_local):
            return rows_all.at[c, pl.ds(b * tok_local + first, count), :]

        def move(kind, c):
            own = x_ref.at[:, pl.ds(c * piece, piece)]
            src, dst, device = [
                (own, block(c, 1), after),
                (own, block(c, 2), before),
                (own, block(c, 4), sibling),
                (block(c, 1, 0, half), block(c, 3, 0, half), after),
                (block(c, 2, half, half), block(c, 3, half, half), before),
                (block(c, 1), block(c, 5), sibling),
                (block(c, 2), block(c, 6), sibling),
                (block(c, 3, 0, half), block(c, 7, 0, half), sibling),
                (block(c, 3, half, half), block(c, 7, half, half), sibling)][kind]
            return remote(src, dst, send_sem.at[kind, c], recv_sem.at[kind, c], device)

        def send_own(c):
            for kind in (0, 1, 2):
                move(kind, c).start()

        def pass_on(c):
            move(0, c).wait_recv()
            move(3, c).start()
            move(5, c).start()
            move(1, c).wait_recv()
            move(4, c).start()
            move(6, c).start()

        def pass_opposite(c):
            move(3, c).wait_recv()
            move(7, c).start()
            move(4, c).wait_recv()
            move(8, c).start()

        def take_rest(c):
            for kind in (2, 5, 6, 7, 8):
                move(kind, c).wait_recv()

        send_own(0)
        send_own(1)
        meta_all[0] = meta_ref[...]
        for c in range(chunks):
            rows_all[c, 0:tok_local, :] = x_ref[:, c * piece:(c + 1) * piece]
        for copy in meta_copies:
            copy.wait_recv()

        def rows(first):
            return jnp.concatenate([meta_all[b, first:first + 8, h * LANES:(h + 1) * LANES] for b in range(ep_size) for h in range(halves)], axis=0)

        local_e = rows(0) - (me * local_experts).astype(F32)
        prio = rows(8)
        gates = rows(16)
        mine = (local_e >= 0.0) & (local_e < float(local_experts))
        mine_prio = jnp.where(mine, prio, 1.0e9)
        thresh = jnp.zeros((1, 1), F32)
        bit = 1
        while bit < n_rows * LANES:
            bit *= 2
        while bit >= 1:
            trial = thresh + float(bit)
            count = jnp.sum(jnp.where(mine_prio < trial, 1.0, 0.0), keepdims=True).reshape(1, 1)
            thresh = jnp.where(count <= float(capacity), trial, thresh)
            bit //= 2
        kept = mine & (prio < thresh)
        row_i = lax.broadcasted_iota(I32, (LANES, LANES), 0)
        col_i = lax.broadcasted_iota(I32, (LANES, LANES), 1)
        upper = jnp.where(row_i < col_i, 1.0, 0.0).astype(BF16)
        lower_r = lax.broadcasted_iota(I32, (n_rows, n_rows), 0)
        lower_c = lax.broadcasted_iota(I32, (n_rows, n_rows), 1)
        lower = jnp.where(lower_c < lower_r, 1.0, 0.0).astype(BF16)
        span_lane = lax.broadcasted_iota(I32, (1, LANES), 1)
        pos = jnp.full((n_rows, LANES), -1.0, F32)
        start = jnp.zeros((1, 1), F32)
        starts = []
        spans = jnp.zeros((1, LANES), F32)
        for e in range(local_experts):
            hit = kept & (local_e == float(e))
            ones = jnp.where(hit, 1.0, 0.0)
            ones16 = ones.astype(BF16)
            in_row = jnp.dot(ones16, upper, preferred_element_type=F32)
            above = jnp.sum(jnp.dot(lower, ones16, preferred_element_type=F32), axis=1, keepdims=True)
            pos = jnp.where(hit, start + in_row + above, pos)
            count = jnp.sum(ones, keepdims=True).reshape(1, 1)
            starts.append(start)
            spans = jnp.where(span_lane == e, start, spans)
            spans = jnp.where(span_lane == local_experts + e, count, spans)
            start = start + jnp.floor((count + float(ALIGN - 1)) * (1.0 / ALIGN)) * float(ALIGN)
            of_e = jnp.where(hit, gates, 0.0)
            for t in range(tok_tiles):
                gate_rows[e:e + 1, t * LANES:(t + 1) * LANES] = jnp.sum(of_e[t * 8:t * 8 + 8, :], axis=0, keepdims=True)
        pos_scr[...] = pos
        span_ref[...] = spans.astype(I32)

        def build(i, carry):
            s_id = (row_i + i * LANES).astype(F32)
            for t in range(tok_tiles):
                any_hit = None
                for k in range(6):
                    r = t * 8 + k
                    eq = pos_scr[r:r + 1, :] == s_id
                    any_hit = eq if any_hit is None else any_hit | eq
                sel[pl.ds(pl.multiple_of(i * LANES, LANES), LANES), t * LANES:(t + 1) * LANES] = jnp.where(any_hit, 1.0, 0.0).astype(BF16)
            return carry

        pass_on(0)
        send_own(2)
        third = slot_tiles // 3
        lax.fori_loop(0, third, build, 0)
        pass_on(1)
        send_own(3)
        lax.fori_loop(third, 2 * third, build, 0)
        pass_opposite(0)
        lax.fori_loop(2 * third, slot_tiles, build, 0)
        pass_on(2)
        send_own(4)

        g32 = gate_rows[...]
        g_hi = g32.astype(BF16)
        rest = g32 - g_hi.astype(F32)
        g_mid = rest.astype(BF16)
        g_lo = (rest - g_mid.astype(F32)).astype(BF16)
        tok_i = lax.broadcasted_iota(I32, (8, n_tokens), 1)
        kind_i = lax.broadcasted_iota(I32, (8, n_tokens), 0)
        numbers = jnp.where(kind_i == 0, tok_i // ALIGN, jnp.where(kind_i == 1, lax.rem(tok_i, ALIGN), 1)).astype(F32).astype(BF16)
        table = jnp.concatenate([g_hi.astype(F32), g_mid.astype(F32), g_lo.astype(F32), numbers.astype(F32)], axis=0).astype(BF16)
        aux_scr[...] = lax.dot_general(sel[...], table, (((1,), (1,)), ((), ())), preferred_element_type=F32)
        eye = row_i == col_i
        lane32 = lax.broadcasted_iota(I32, (LANES, 32), 1)
        sub32 = lax.broadcasted_iota(I32, (LANES, 32), 0)

        def table_row(i, carry):
            aux = aux_scr[pl.ds(pl.multiple_of(i * LANES, LANES), LANES), :]
            s_id = (sub32 + i * LANES).astype(F32)
            owner = jnp.zeros((LANES, 32), F32)
            for e in range(1, local_experts):
                owner = owner + jnp.where(s_id >= starts[e], 1.0, 0.0)
            is_gate = (lane32 < 24) & (lax.rem(lane32, 8).astype(F32) == owner)
            gate_col = jnp.sum(jnp.where(is_gate, aux, 0.0), axis=1, keepdims=True)
            tok_w = jnp.where(lane32 == 24, float(ALIGN), jnp.where(lane32 == 25, 1.0, 0.0))
            hit_col = jnp.sum(jnp.where(lane32 == 26, aux, 0.0), axis=1, keepdims=True)
            tok_col = jnp.sum(aux * tok_w, axis=1, keepdims=True)
            tok_col = jnp.where(hit_col > 0.5, tok_col, float(n_tokens))
            tok_ref[pl.ds(i, 1), :] = jnp.sum(jnp.where(eye, tok_col, 0.0), axis=0, keepdims=True).astype(I32)
            gate_ref[pl.ds(i, 1), :] = jnp.sum(jnp.where(eye, gate_col, 0.0), axis=0, keepdims=True)
            return carry

        lax.fori_loop(0, slot_tiles, table_row, 0)

        def out_copy(c):
            return pltpu.make_async_copy(picked.at[c % 2], out_ref.at[pl.ds(0, used), pl.ds(c * piece, piece)], out_sem.at[c % 2])

        def pick(c):
            take_rest(c)
            if c >= 2:
                out_copy(c - 2).wait()

            def step(i, carry):
                at = pl.ds(pl.multiple_of(i * sel_step, ALIGN), sel_step)
                picked[c % 2, at, :] = jnp.dot(sel[at, :], rows_all[c], preferred_element_type=F32).astype(BF16)
                return carry

            lax.fori_loop(0, used // sel_step, step, 0)
            out_copy(c).start()

        pass_opposite(1)
        pick(0)
        pass_on(3)
        pass_opposite(2)
        pick(1)
        pass_on(4)
        pass_opposite(3)
        pick(2)
        pass_opposite(4)
        pick(3)
        pick(4)
        out_copy(3).wait()
        out_copy(4).wait()
        for copy in meta_copies:
            copy.wait_send()
        for c in range(chunks):
            for kind in range(9):
                move(kind, c).wait_send()

    vmem = pl.BlockSpec(memory_space=pltpu.VMEM)
    dma = pltpu.SemaphoreType.DMA
    table_rows = -(-slot_tiles // 8) * 8
    return pl.pallas_call(
        kernel,
        out_shape=(
            pltpu.HBM((slots, width), BF16),
            jax.ShapeDtypeStruct((table_rows, LANES), I32),
            jax.ShapeDtypeStruct((table_rows, LANES), F32),
            jax.ShapeDtypeStruct((1, LANES), I32)),
        in_specs=[vmem, vmem],
        out_specs=(pl.BlockSpec(memory_space=pltpu.HBM), vmem, vmem, vmem),
        scratch_shapes=[
            pltpu.VMEM((ep_size, meta_rows, tok_local), F32), pltpu.VMEM((chunks, n_tokens, piece), BF16),
            pltpu.VMEM((used, n_tokens), BF16), pltpu.VMEM((2, used, piece), BF16),
            pltpu.VMEM((n_rows, LANES), F32), pltpu.VMEM((local_experts, n_tokens), F32), pltpu.VMEM((used, 32), F32),
            dma((len(moves),)), dma((len(moves),)), dma((9, chunks)), dma((9, chunks)), dma((2,))],
        compiler_params=pltpu.CompilerParams(collective_id=0, has_side_effects=True, vmem_limit_bytes=36 * 1024 * 1024),
        name='dispatch',
    )(meta, normed)


def experts(spans, slot_tok, slot_gate, rows_in, expert_w1, expert_w3, expert_w2, n_tokens, capacity):
    slots, width = rows_in.shape
    local_experts, _, ff = expert_w1.shape
    groups = width // LANES
    up_cols, n_up = 512, ff // 512
    down_cols, n_down = width // 2, 2
    down_groups = down_cols // LANES
    max_items = local_experts + -(-capacity // ROW_TILE)
    acc_rows = (n_tokens + 8) * groups
    sizes = (128, 160, 192, 224, 256)
    batch = 8

    def kernel(span_ref, tok_ref, gate_ref, x_ref, w1_ref, w3_ref, w2_ref, acc,
               row_scr, hid, x_tile, up, down, item_e, item_base, item_count, x_sem, up_sem, down_sem):
        def plan(e, n):
            count = span_ref[local_experts + e]

            def one(j, m):
                item_e[m] = e
                item_base[m] = span_ref[e] + j * ROW_TILE
                item_count[m] = jnp.minimum(count - j * ROW_TILE, ROW_TILE)
                return m + 1

            return lax.fori_loop(0, (count + ROW_TILE - 1) // ROW_TILE, one, n)

        n_items = lax.fori_loop(0, local_experts, plan, 0)

        def x_copy(i, slot):
            return pltpu.make_async_copy(x_ref.at[pl.ds(pl.multiple_of(item_base[i], ALIGN), ROW_TILE), :], x_tile.at[slot], x_sem.at[slot])

        def up_copy(i, k, which):
            src = w1_ref if which == 0 else w3_ref
            return pltpu.make_async_copy(src.at[item_e[i], :, pl.ds(k * up_cols, up_cols)], up.at[k, which], up_sem.at[k, which])

        def down_copy(i, k):
            return pltpu.make_async_copy(w2_ref.at[item_e[i], :, pl.ds(k * down_cols, down_cols)], down.at[k], down_sem.at[k])

        @pl.when(n_items > 0)
        def _():
            x_copy(0, 0).start()
            for k in range(n_up):
                up_copy(0, k, 0).start()
                up_copy(0, k, 1).start()
            for k in range(n_down):
                down_copy(0, k).start()

        def zero(i, carry):
            acc[pl.ds(pl.multiple_of(i * groups * 8, 8), groups * 8), :] = jnp.zeros((groups * 8, LANES), F32)
            return carry

        lax.fori_loop(0, acc_rows // (groups * 8), zero, 0)

        def item(i, carry):
            slot = lax.rem(i, 2)
            base = item_base[i]
            count = item_count[i]
            more = i + 1 < n_items
            x_copy(i, slot).wait()

            @pl.when(more)
            def _():
                x_copy(i + 1, 1 - slot).start()

            def sized(body):
                low = 0
                for size in sizes:
                    pl.when((count > low) & (count <= size))(functools.partial(body, size))
                    low = size

            for k in range(n_up):
                up_copy(i, k, 0).wait()
                up_copy(i, k, 1).wait()

                def up_part(size, k=k):
                    x = x_tile[slot, :size, :]
                    up_a = jnp.dot(x, up[k, 0], preferred_element_type=F32)
                    up_b = jnp.dot(x, up[k, 1], preferred_element_type=F32)
                    hid[:size, k * up_cols:(k + 1) * up_cols] = (jax.nn.silu(up_a) * up_b).astype(BF16)

                sized(up_part)

                @pl.when(more)
                def _(k=k):
                    up_copy(i + 1, k, 0).start()
                    up_copy(i + 1, k, 1).start()

            for k in range(n_down):
                down_copy(i, k).wait()

                def down_part(size, k=k):
                    out = jnp.dot(hid[:size, :], down[k], preferred_element_type=F32).astype(BF16).astype(F32)
                    for g in range(down_groups):
                        row_scr[pl.ds(k * down_groups + g, size, stride=groups), :] = out[:, g * LANES:(g + 1) * LANES]

                sized(down_part)

                @pl.when(more)
                def _(k=k):
                    down_copy(i + 1, k).start()

            def add_rows(q, inner):
                ats, new = [], []
                for u in range(batch):
                    s = base + q * batch + u
                    at = pl.ds(tok_ref[s] * groups, groups)
                    ats.append(at)
                    new.append(acc[at, :] + gate_ref[s] * row_scr[pl.ds((q * batch + u) * groups, groups), :])
                for at, value in zip(ats, new):
                    acc[at, :] = value
                return inner

            lax.fori_loop(0, (count + batch - 1) // batch, add_rows, 0)
            return carry

        lax.fori_loop(0, n_items, item, 0)

    hbm = pl.BlockSpec(memory_space=pl.ANY)
    dma = pltpu.SemaphoreType.DMA
    return pl.pallas_call(
        kernel,
        out_shape=pltpu.VMEM((acc_rows, LANES), F32),
        grid_spec=pltpu.PrefetchScalarGridSpec(
            num_scalar_prefetch=3, grid=(), in_specs=[hbm] * 4, out_specs=pl.BlockSpec(memory_space=pltpu.VMEM),
            scratch_shapes=[
                pltpu.VMEM((ROW_TILE * groups, LANES), F32),
                pltpu.VMEM((ROW_TILE, ff), BF16), pltpu.VMEM((2, ROW_TILE, width), BF16),
                pltpu.VMEM((n_up, 2, width, up_cols), BF16), pltpu.VMEM((n_down, ff, down_cols), BF16),
                pltpu.SMEM((max_items,), I32), pltpu.SMEM((max_items,), I32), pltpu.SMEM((max_items,), I32),
                dma((2,)), dma((n_up, 2)), dma((n_down,))]),
        compiler_params=pltpu.CompilerParams(vmem_limit_bytes=34 * 1024 * 1024),
        cost_estimate=pl.CostEstimate(flops=6 * capacity * width * ff, bytes_accessed=6 * local_experts * width * ff, transcendentals=capacity * ff),
        name='experts',
    )(spans, slot_tok, slot_gate, rows_in, expert_w1, expert_w3, expert_w2)


def reduce_and_finish(sums, resid_in, normed, shared_w1, shared_w3, shared_w2, ep_size):
    chips = ep_size // 2
    tok_local, width = resid_in.shape
    ff = shared_w1.shape[1]
    groups = width // LANES
    pieces = 4
    tok_piece = tok_local // pieces
    piece_rows = tok_piece * groups
    up_cols = 256
    n_up = ff // up_cols
    down_cols = 256
    n_down = width // down_cols
    add_step = 128

    def kernel(sums_ref, resid_ref, x_ref, w1_ref, w3_ref, w2_ref, out_ref,
               pair, opp, home, up_buf, down_buf, hid, shared,
               pair_send, pair_recv, fwd_send, fwd_recv, bwd_send, bwd_recv, up_sem, down_sem):
        me = lax.axis_index('ep')
        chip, core = me // 2, lax.rem(me, 2)
        sibling = 2 * chip + 1 - core
        after = 2 * lax.rem(chip + 1, chips) + core
        before = 2 * lax.rem(chip + chips - 1, chips) + core

        def up_copy(j, slot, which):
            src = w1_ref if which == 0 else w3_ref
            return pltpu.make_async_copy(src.at[:, pl.ds(pl.multiple_of(j * up_cols, LANES), up_cols)], up_buf.at[slot, which], up_sem.at[slot, which])

        def down_copy(j, slot):
            return pltpu.make_async_copy(w2_ref.at[:, pl.ds(pl.multiple_of(j * down_cols, LANES), down_cols)], down_buf.at[slot], down_sem.at[slot])

        barrier = pltpu.get_barrier_semaphore()
        for peer in (sibling, after, before):
            pl.semaphore_signal(barrier, inc=1, device_id={'ep': peer}, device_id_type=pl.DeviceIdType.MESH)
        pl.semaphore_wait(barrier, 3)

        def block_piece(b, q):
            return sums_ref.at[pl.ds((b * pieces + q) * piece_rows, piece_rows), :]

        def to_pair(o, q):
            return pltpu.make_async_remote_copy(
                src_ref=block_piece(chips + o, q), dst_ref=pair.at[o, q], send_sem=pair_send.at[o, q], recv_sem=pair_recv.at[o, q],
                device_id={'ep': sibling}, device_id_type=pl.DeviceIdType.MESH)

        def ring(src, dst, send, recv, i, peer):
            return pltpu.make_async_remote_copy(
                src_ref=src, dst_ref=dst, send_sem=send.at[i], recv_sem=recv.at[i],
                device_id={'ep': peer}, device_id_type=pl.DeviceIdType.MESH)

        order = [(o, q) for o in (3, 2, 1, 0) for q in ((0, 2, 1, 3) if o == 3 else (2, 3, 0, 1) if o == 2 else (0, 1, 2, 3))]
        for o, q in order:
            to_pair(o, q).start()
        for slot in range(2):
            for which in range(2):
                up_copy(slot, slot, which).start()

        def add(o, q, src):
            def step(i, carry):
                at = pl.ds(pl.multiple_of(i * add_step, add_step), add_step)
                pair[o, q, at, :] = pair[o, q, at, :] + src[at, :]
                return carry

            lax.fori_loop(0, piece_rows // add_step, step, 0)

        def pair_sum(o, q):
            to_pair(o, q).wait_recv()
            add(o, q, block_piece(o, q))

        opp_fwd = [ring(pair.at[3, q], opp.at[q], fwd_send, fwd_recv, q, after) for q in (0, 1)]
        opp_bwd = [ring(pair.at[3, 2 + q], opp.at[2 + q], bwd_send, bwd_recv, q, before) for q in (0, 1)]
        home_fwd = {q: ring(pair.at[2, q], home.at[0, q], fwd_send, fwd_recv, 2 + q, after) for q in range(pieces)}
        home_bwd = {q: ring(pair.at[1, q], home.at[1, q], bwd_send, bwd_recv, 2 + q, before) for q in range(pieces)}
        for q in (0, 1):
            pair_sum(3, q)
            pair_sum(3, 2 + q)
            opp_fwd[q].start()
            opp_bwd[q].start()
        for q in (0, 1):
            pair_sum(2, 2 + q)
            pair_sum(1, q)
            home_fwd[2 + q].start()
            home_bwd[q].start()
        for q in (0, 1):
            pair_sum(2, q)
            pair_sum(1, 2 + q)

        def up_step(j, carry):
            slot = lax.rem(j, 2)
            up_copy(j, slot, 0).wait()
            up_copy(j, slot, 1).wait()
            up_a = jnp.dot(x_ref[...], up_buf[slot, 0], preferred_element_type=F32)
            up_b = jnp.dot(x_ref[...], up_buf[slot, 1], preferred_element_type=F32)
            hid[:, pl.ds(pl.multiple_of(j * up_cols, LANES), up_cols)] = (jax.nn.silu(up_a) * up_b).astype(BF16)

            @pl.when(j + 2 < n_up)
            def _():
                up_copy(j + 2, slot, 0).start()
                up_copy(j + 2, slot, 1).start()

            return carry

        for slot in range(2):
            down_copy(slot, slot).start()
        lax.fori_loop(0, n_up, up_step, 0)

        def down_step(j, carry):
            slot = lax.rem(j, 2)
            down_copy(j, slot).wait()
            part = jnp.dot(hid[...], down_buf[slot], preferred_element_type=F32)
            shared[:, pl.ds(pl.multiple_of(j * down_cols, LANES), down_cols)] = part.astype(BF16)

            @pl.when(j + 2 < n_down)
            def _():
                down_copy(j + 2, slot).start()

            return carry

        lax.fori_loop(0, n_down, down_step, 0)

        for q in range(pieces):
            pair_sum(0, q)
        for q in (0, 1):
            opp_fwd[q].wait_recv()
            add(2, q, opp.at[q])
            home_fwd[q].start()
            opp_bwd[q].wait_recv()
            add(1, 2 + q, opp.at[2 + q])
            home_bwd[2 + q].start()
        for q in (0, 1):
            home_fwd[2 + q].wait_recv()
            add(0, 2 + q, home.at[0, 2 + q])
            home_bwd[q].wait_recv()
            add(0, q, home.at[1, q])
        for q in (0, 2, 1, 3):
            way, late = (0, home_fwd[q]) if q < 2 else (1, home_bwd[q])
            late.wait_recv()
            rows = slice(q * tok_piece, (q + 1) * tok_piece)
            for g in range(groups):
                col = g * LANES
                at = pl.ds(g, tok_piece, stride=groups)
                routed = pair[0, q, at, :] + home[way, q, at, :]
                total = resid_ref[rows, col:col + LANES].astype(F32) + shared[rows, col:col + LANES].astype(F32) + routed
                out_ref[rows, col:col + LANES] = total.astype(BF16)
        for o, q in order:
            to_pair(o, q).wait_send()
        for copy in opp_fwd + opp_bwd + list(home_fwd.values()) + list(home_bwd.values()):
            copy.wait_send()

    hbm = pl.BlockSpec(memory_space=pl.ANY)
    vmem = pl.BlockSpec(memory_space=pltpu.VMEM)
    dma = pltpu.SemaphoreType.DMA
    return pl.pallas_call(
        kernel,
        out_shape=pltpu.VMEM((tok_local, width), BF16),
        in_specs=[vmem, vmem, vmem, hbm, hbm, hbm],
        out_specs=vmem,
        scratch_shapes=[
            pltpu.VMEM((chips, pieces, piece_rows, LANES), F32),
            pltpu.VMEM((pieces, piece_rows, LANES), F32), pltpu.VMEM((2, pieces, piece_rows, LANES), F32),
            pltpu.VMEM((2, 2, width, up_cols), BF16), pltpu.VMEM((2, ff, down_cols), BF16),
            pltpu.VMEM((tok_local, ff), BF16), pltpu.VMEM((tok_local, width), BF16),
            dma((chips, pieces)), dma((chips, pieces)), dma((6,)), dma((6,)), dma((6,)), dma((6,)), dma((2, 2)), dma((2,))],
        compiler_params=pltpu.CompilerParams(collective_id=1, has_side_effects=True, vmem_limit_bytes=37 * 1024 * 1024),
        cost_estimate=pl.CostEstimate(flops=6 * tok_local * width * ff, bytes_accessed=6 * width * ff, transcendentals=tok_local * ff),
        name='reduce_and_finish',
    )(pltpu.with_memory_space_constraint(sums, pltpu.VMEM), resid_in, normed, shared_w1, shared_w3, shared_w2)


def solution(mesh):
    ep_size = mesh.shape['ep']
    tok_spec = P(('dp', 'ep'))
    expert_spec = P('ep')

    def device_fn(resid_in, expert_ids, priority, norm_gain, router_w, shared_w1, shared_w3, shared_w2, expert_w1, expert_w3, expert_w2):
        tok_local, width = resid_in.shape
        top_k = expert_ids.shape[1]
        local_experts = expert_w1.shape[0]
        capacity = tok_local * top_k
        n_tokens = tok_local * ep_size
        slots = -(-(capacity + local_experts * ALIGN + ROW_TILE) // LANES) * LANES
        normed, meta = norm_and_gates(resid_in, norm_gain, router_w.T, expert_ids.T, priority.T)
        rows_in, slot_tok, slot_gate, spans = dispatch(meta, normed, local_experts, capacity, slots, ep_size)
        spans = spans.reshape(-1)
        sums = experts(spans, slot_tok.reshape(-1), slot_gate.reshape(-1), rows_in, expert_w1, expert_w3, expert_w2, n_tokens, capacity)
        return reduce_and_finish(sums, resid_in, normed, shared_w1, shared_w3, shared_w2, ep_size)

    return jax.shard_map(device_fn, mesh=mesh, in_specs=(tok_spec, tok_spec, tok_spec, P(), P(), P(), P(), P(), expert_spec, expert_spec, expert_spec), out_specs=tok_spec, check_vma=False)
```

```python
import functools
import jax
import jax.numpy as jnp
from jax import lax
from jax.experimental import pallas as pl
from jax.experimental.pallas import tpu as pltpu
from jax.sharding import PartitionSpec as P

NORM_EPS = 1e-6
ROUTE_SCALE = 16.0
LANES = 128
ROW_TILE = 256
ALIGN = 16
F32, BF16, I32 = jnp.float32, jnp.bfloat16, jnp.int32


def norm_and_gates(resid_in, norm_gain, router_t, ids_t, prio_t):
    tok_local, width = resid_in.shape
    top_k = ids_t.shape[0]
    n_experts = router_t.shape[0]

    def kernel(resid_hbm, gain_hbm, router_hbm, ids_hbm, prio_hbm, x_ref, meta_ref, resid_ref, gain_ref, router_ref, ids_ref, prio_ref, sem):
        pairs = ((resid_hbm, resid_ref), (gain_hbm, gain_ref), (router_hbm, router_ref), (ids_hbm, ids_ref), (prio_hbm, prio_ref))
        copies = [pltpu.make_async_copy(src, dst, sem.at[i]) for i, (src, dst) in enumerate(pairs)]
        for copy in copies:
            copy.start()
        for copy in copies:
            copy.wait()
        resid32 = resid_ref[...].astype(F32)
        inv_rms = lax.rsqrt(jnp.mean(resid32 * resid32, axis=1, keepdims=True) + NORM_EPS)
        normed = (resid32 * inv_rms * gain_ref[...]).astype(BF16)
        x_ref[...] = normed
        logits = lax.dot_general(normed, router_ref[...], (((1,), (1,)), ((), ())), preferred_element_type=F32)
        powers = jnp.exp(logits - jnp.max(logits, axis=1, keepdims=True))
        probs = powers / jnp.sum(powers, axis=1, keepdims=True)
        meta_ref[0:8, :] = jnp.full((8, tok_local), -1.0e6, F32)
        meta_ref[8:, :] = jnp.zeros((16, tok_local), F32)
        meta_ref[0:top_k, :] = ids_ref[...].astype(F32)
        meta_ref[8:8 + top_k, :] = prio_ref[...].astype(F32)
        eye = lax.broadcasted_iota(I32, (LANES, LANES), 0) == lax.broadcasted_iota(I32, (LANES, LANES), 1)
        expert = lax.broadcasted_iota(I32, (LANES, n_experts), 1).astype(F32)
        for h in range(tok_local // LANES):
            span = slice(h * LANES, (h + 1) * LANES)
            for k in range(top_k):
                id_col = jnp.sum(jnp.where(eye, ids_ref[k:k + 1, span].astype(F32), 0.0), axis=1, keepdims=True)
                gate_col = ROUTE_SCALE * jnp.sum(jnp.where(expert == id_col, probs[span, :], 0.0), axis=1, keepdims=True)
                meta_ref[16 + k:17 + k, span] = jnp.sum(jnp.where(eye, gate_col, 0.0), axis=0, keepdims=True)

    vmem = pl.BlockSpec(memory_space=pltpu.VMEM)
    return pl.pallas_call(
        kernel,
        out_shape=(jax.ShapeDtypeStruct((tok_local, width), BF16), jax.ShapeDtypeStruct((24, tok_local), F32)),
        in_specs=[pl.BlockSpec(memory_space=pltpu.HBM)] * 5, out_specs=(vmem, vmem),
        scratch_shapes=[pltpu.VMEM(resid_in.shape, BF16), pltpu.VMEM((1, width), F32), pltpu.VMEM(router_t.shape, BF16),
                        pltpu.VMEM(ids_t.shape, I32), pltpu.VMEM(prio_t.shape, I32), pltpu.SemaphoreType.DMA((5,))],
        compiler_params=pltpu.CompilerParams(vmem_limit_bytes=30 * 1024 * 1024),
        name='norm_and_gates',
    )(*[pltpu.with_memory_space_constraint(x, pltpu.HBM) for x in (resid_in, norm_gain.reshape(1, width), router_t, ids_t, prio_t)])


def dispatch(meta, normed, local_experts, capacity, slots, ep_size):
    meta_rows, tok_local = meta.shape
    width = normed.shape[1]
    chips = ep_size // 2
    n_tokens = ep_size * tok_local
    half = tok_local // 2
    chunks = 5
    piece = width // chunks
    halves = tok_local // LANES
    tok_tiles = ep_size * halves
    n_rows = tok_tiles * 8
    used = capacity + local_experts * ALIGN
    slot_tiles = used // LANES
    sel_step = used // 2
    moves = [(dc, ds) for ds in range(2) for dc in range(chips) if (dc, ds) != (0, 0)]
    seen_from = {0: 0, 1: 1, chips - 1: 2, 2: 3}

    def kernel(meta_ref, x_ref, out_ref, tok_ref, gate_ref, span_ref,
               meta_all, rows_all, sel, picked, pos_scr, gate_rows, aux_scr,
               meta_send, meta_recv, send_sem, recv_sem, out_sem):
        me = lax.axis_index('ep')
        chip, core = me // 2, lax.rem(me, 2)

        def peer(dc, ds):
            return 2 * lax.rem(chip + dc, chips) + (core if ds == 0 else 1 - core)

        sibling, after, before = peer(0, 1), peer(1, 0), peer(chips - 1, 0)

        def remote(src, dst, send, recv, device):
            return pltpu.make_async_remote_copy(src_ref=src, dst_ref=dst, send_sem=send, recv_sem=recv,
                                                device_id={'ep': device}, device_id_type=pl.DeviceIdType.MESH)

        barrier = pltpu.get_barrier_semaphore()
        for dc, ds in moves:
            pl.semaphore_signal(barrier, inc=1, device_id={'ep': peer(dc, ds)}, device_id_type=pl.DeviceIdType.MESH)
        pl.semaphore_wait(barrier, len(moves))

        meta_copies = [remote(meta_ref, meta_all.at[4 * ds + seen_from[dc]], meta_send.at[i], meta_recv.at[i], peer(dc, ds))
                       for i, (dc, ds) in enumerate(moves)]
        for copy in meta_copies:
            copy.start()

        def block(c, b, first=0, count=tok_local):
            return rows_all.at[c, pl.ds(b * tok_local + first, count), :]

        def move(kind, c):
            own = x_ref.at[:, pl.ds(c * piece, piece)]
            src, dst, device = [
                (own, block(c, 1), after),
                (own, block(c, 2), before),
                (own, block(c, 4), sibling),
                (block(c, 1, 0, half), block(c, 3, 0, half), after),
                (block(c, 2, half, half), block(c, 3, half, half), before),
                (block(c, 1), block(c, 5), sibling),
                (block(c, 2), block(c, 6), sibling),
                (block(c, 3, 0, half), block(c, 7, 0, half), sibling),
                (block(c, 3, half, half), block(c, 7, half, half), sibling)][kind]
            return remote(src, dst, send_sem.at[kind, c], recv_sem.at[kind, c], device)

        def send_own(c):
            for kind in (0, 1, 2):
                move(kind, c).start()

        def pass_on(c):
            move(0, c).wait_recv()
            move(3, c).start()
            move(5, c).start()
            move(1, c).wait_recv()
            move(4, c).start()
            move(6, c).start()

        def pass_opposite(c):
            move(3, c).wait_recv()
            move(7, c).start()
            move(4, c).wait_recv()
            move(8, c).start()

        def take_rest(c):
            for kind in (2, 5, 6, 7, 8):
                move(kind, c).wait_recv()

        send_own(0)
        send_own(1)
        meta_all[0] = meta_ref[...]
        for c in range(chunks):
            rows_all[c, 0:tok_local, :] = x_ref[:, c * piece:(c + 1) * piece]
        for copy in meta_copies:
            copy.wait_recv()

        def rows(first):
            return jnp.concatenate([meta_all[b, first:first + 8, h * LANES:(h + 1) * LANES] for b in range(ep_size) for h in range(halves)], axis=0)

        local_e = rows(0) - (me * local_experts).astype(F32)
        prio = rows(8)
        gates = rows(16)
        mine = (local_e >= 0.0) & (local_e < float(local_experts))
        mine_prio = jnp.where(mine, prio, 1.0e9)
        thresh = jnp.zeros((1, 1), F32)
        bit = 1
        while bit < n_rows * LANES:
            bit *= 2
        while bit >= 1:
            trial = thresh + float(bit)
            count = jnp.sum(jnp.where(mine_prio < trial, 1.0, 0.0), keepdims=True).reshape(1, 1)
            thresh = jnp.where(count <= float(capacity), trial, thresh)
            bit //= 2
        kept = mine & (prio < thresh)
        row_i = lax.broadcasted_iota(I32, (LANES, LANES), 0)
        col_i = lax.broadcasted_iota(I32, (LANES, LANES), 1)
        upper = jnp.where(row_i < col_i, 1.0, 0.0).astype(BF16)
        lower_r = lax.broadcasted_iota(I32, (n_rows, n_rows), 0)
        lower_c = lax.broadcasted_iota(I32, (n_rows, n_rows), 1)
        lower = jnp.where(lower_c < lower_r, 1.0, 0.0).astype(BF16)
        span_lane = lax.broadcasted_iota(I32, (1, LANES), 1)
        pos = jnp.full((n_rows, LANES), -1.0, F32)
        start = jnp.zeros((1, 1), F32)
        starts = []
        spans = jnp.zeros((1, LANES), F32)
        for e in range(local_experts):
            hit = kept & (local_e == float(e))
            ones = jnp.where(hit, 1.0, 0.0)
            ones16 = ones.astype(BF16)
            in_row = jnp.dot(ones16, upper, preferred_element_type=F32)
            above = jnp.sum(jnp.dot(lower, ones16, preferred_element_type=F32), axis=1, keepdims=True)
            pos = jnp.where(hit, start + in_row + above, pos)
            count = jnp.sum(ones, keepdims=True).reshape(1, 1)
            starts.append(start)
            spans = jnp.where(span_lane == e, start, spans)
            spans = jnp.where(span_lane == local_experts + e, count, spans)
            start = start + jnp.floor((count + float(ALIGN - 1)) * (1.0 / ALIGN)) * float(ALIGN)
            of_e = jnp.where(hit, gates, 0.0)
            for t in range(tok_tiles):
                gate_rows[e:e + 1, t * LANES:(t + 1) * LANES] = jnp.sum(of_e[t * 8:t * 8 + 8, :], axis=0, keepdims=True)
        pos_scr[...] = pos
        span_ref[...] = spans.astype(I32)

        def build(i, carry):
            s_id = (row_i + i * LANES).astype(F32)
            for t in range(tok_tiles):
                any_hit = None
                for k in range(6):
                    r = t * 8 + k
                    eq = pos_scr[r:r + 1, :] == s_id
                    any_hit = eq if any_hit is None else any_hit | eq
                sel[pl.ds(pl.multiple_of(i * LANES, LANES), LANES), t * LANES:(t + 1) * LANES] = jnp.where(any_hit, 1.0, 0.0).astype(BF16)
            return carry

        pass_on(0)
        send_own(2)
        third = slot_tiles // 3
        lax.fori_loop(0, third, build, 0)
        pass_on(1)
        send_own(3)
        lax.fori_loop(third, 2 * third, build, 0)
        pass_opposite(0)
        lax.fori_loop(2 * third, slot_tiles, build, 0)
        pass_on(2)
        send_own(4)

        g32 = gate_rows[...]
        g_hi = g32.astype(BF16)
        rest = g32 - g_hi.astype(F32)
        g_mid = rest.astype(BF16)
        g_lo = (rest - g_mid.astype(F32)).astype(BF16)
        tok_i = lax.broadcasted_iota(I32, (8, n_tokens), 1)
        kind_i = lax.broadcasted_iota(I32, (8, n_tokens), 0)
        numbers = jnp.where(kind_i == 0, tok_i // ALIGN, jnp.where(kind_i == 1, lax.rem(tok_i, ALIGN), 1)).astype(F32).astype(BF16)
        table = jnp.concatenate([g_hi.astype(F32), g_mid.astype(F32), g_lo.astype(F32), numbers.astype(F32)], axis=0).astype(BF16)
        aux_scr[...] = lax.dot_general(sel[...], table, (((1,), (1,)), ((), ())), preferred_element_type=F32)
        eye = row_i == col_i
        lane32 = lax.broadcasted_iota(I32, (LANES, 32), 1)
        sub32 = lax.broadcasted_iota(I32, (LANES, 32), 0)

        def table_row(i, carry):
            aux = aux_scr[pl.ds(pl.multiple_of(i * LANES, LANES), LANES), :]
            s_id = (sub32 + i * LANES).astype(F32)
            owner = jnp.zeros((LANES, 32), F32)
            for e in range(1, local_experts):
                owner = owner + jnp.where(s_id >= starts[e], 1.0, 0.0)
            is_gate = (lane32 < 24) & (lax.rem(lane32, 8).astype(F32) == owner)
            gate_col = jnp.sum(jnp.where(is_gate, aux, 0.0), axis=1, keepdims=True)
            tok_w = jnp.where(lane32 == 24, float(ALIGN), jnp.where(lane32 == 25, 1.0, 0.0))
            hit_col = jnp.sum(jnp.where(lane32 == 26, aux, 0.0), axis=1, keepdims=True)
            tok_col = jnp.sum(aux * tok_w, axis=1, keepdims=True)
            tok_col = jnp.where(hit_col > 0.5, tok_col, float(n_tokens))
            tok_ref[pl.ds(i, 1), :] = jnp.sum(jnp.where(eye, tok_col, 0.0), axis=0, keepdims=True).astype(I32)
            gate_ref[pl.ds(i, 1), :] = jnp.sum(jnp.where(eye, gate_col, 0.0), axis=0, keepdims=True)
            return carry

        lax.fori_loop(0, slot_tiles, table_row, 0)

        def out_copy(c):
            return pltpu.make_async_copy(picked.at[c % 2], out_ref.at[pl.ds(0, used), pl.ds(c * piece, piece)], out_sem.at[c % 2])

        def pick(c):
            take_rest(c)
            if c >= 2:
                out_copy(c - 2).wait()

            def step(i, carry):
                at = pl.ds(pl.multiple_of(i * sel_step, ALIGN), sel_step)
                picked[c % 2, at, :] = jnp.dot(sel[at, :], rows_all[c], preferred_element_type=F32).astype(BF16)
                return carry

            lax.fori_loop(0, used // sel_step, step, 0)
            out_copy(c).start()

        pass_opposite(1)
        pick(0)
        pass_on(3)
        pass_opposite(2)
        pick(1)
        pass_on(4)
        pass_opposite(3)
        pick(2)
        pass_opposite(4)
        pick(3)
        pick(4)
        out_copy(3).wait()
        out_copy(4).wait()
        for copy in meta_copies:
            copy.wait_send()
        for c in range(chunks):
            for kind in range(9):
                move(kind, c).wait_send()

    vmem = pl.BlockSpec(memory_space=pltpu.VMEM)
    dma = pltpu.SemaphoreType.DMA
    table_rows = -(-slot_tiles // 8) * 8
    return pl.pallas_call(
        kernel,
        out_shape=(
            pltpu.HBM((slots, width), BF16),
            jax.ShapeDtypeStruct((table_rows, LANES), I32),
            jax.ShapeDtypeStruct((table_rows, LANES), F32),
            jax.ShapeDtypeStruct((1, LANES), I32)),
        in_specs=[vmem, vmem],
        out_specs=(pl.BlockSpec(memory_space=pltpu.HBM), vmem, vmem, vmem),
        scratch_shapes=[
            pltpu.VMEM((ep_size, meta_rows, tok_local), F32), pltpu.VMEM((chunks, n_tokens, piece), BF16),
            pltpu.VMEM((used, n_tokens), BF16), pltpu.VMEM((2, used, piece), BF16),
            pltpu.VMEM((n_rows, LANES), F32), pltpu.VMEM((local_experts, n_tokens), F32), pltpu.VMEM((used, 32), F32),
            dma((len(moves),)), dma((len(moves),)), dma((9, chunks)), dma((9, chunks)), dma((2,))],
        compiler_params=pltpu.CompilerParams(collective_id=0, has_side_effects=True, vmem_limit_bytes=36 * 1024 * 1024),
        name='dispatch',
    )(meta, normed)


def experts(spans, slot_tok, slot_gate, rows_in, expert_w1, expert_w3, expert_w2, n_tokens, capacity):
    slots, width = rows_in.shape
    local_experts, _, ff = expert_w1.shape
    groups = width // LANES
    up_cols, n_up = 512, ff // 512
    down_cols, n_down = width // 2, 2
    down_groups = down_cols // LANES
    max_items = local_experts + -(-capacity // ROW_TILE)
    acc_rows = (n_tokens + 8) * groups
    sizes = (128, 160, 192, 224, 256)
    batch = 8

    def kernel(span_ref, tok_ref, gate_ref, x_ref, w1_ref, w3_ref, w2_ref, acc,
               row_scr, hid, x_tile, up, down, item_e, item_base, item_count, x_sem, up_sem, down_sem):
        def plan(e, n):
            count = span_ref[local_experts + e]

            def one(j, m):
                item_e[m] = e
                item_base[m] = span_ref[e] + j * ROW_TILE
                item_count[m] = jnp.minimum(count - j * ROW_TILE, ROW_TILE)
                return m + 1

            return lax.fori_loop(0, (count + ROW_TILE - 1) // ROW_TILE, one, n)

        n_items = lax.fori_loop(0, local_experts, plan, 0)

        def x_copy(i, slot):
            return pltpu.make_async_copy(x_ref.at[pl.ds(pl.multiple_of(item_base[i], ALIGN), ROW_TILE), :], x_tile.at[slot], x_sem.at[slot])

        def up_copy(i, k, which):
            src = w1_ref if which == 0 else w3_ref
            return pltpu.make_async_copy(src.at[item_e[i], :, pl.ds(k * up_cols, up_cols)], up.at[k, which], up_sem.at[k, which])

        def down_copy(i, k):
            return pltpu.make_async_copy(w2_ref.at[item_e[i], :, pl.ds(k * down_cols, down_cols)], down.at[k], down_sem.at[k])

        @pl.when(n_items > 0)
        def _():
            x_copy(0, 0).start()
            for k in range(n_up):
                up_copy(0, k, 0).start()
                up_copy(0, k, 1).start()
            for k in range(n_down):
                down_copy(0, k).start()

        def zero(i, carry):
            acc[pl.ds(pl.multiple_of(i * groups * 8, 8), groups * 8), :] = jnp.zeros((groups * 8, LANES), F32)
            return carry

        lax.fori_loop(0, acc_rows // (groups * 8), zero, 0)

        def item(i, carry):
            slot = lax.rem(i, 2)
            base = item_base[i]
            count = item_count[i]
            more = i + 1 < n_items
            x_copy(i, slot).wait()

            @pl.when(more)
            def _():
                x_copy(i + 1, 1 - slot).start()

            def sized(body):
                low = 0
                for size in sizes:
                    pl.when((count > low) & (count <= size))(functools.partial(body, size))
                    low = size

            for k in range(n_up):
                up_copy(i, k, 0).wait()
                up_copy(i, k, 1).wait()

                def up_part(size, k=k):
                    x = x_tile[slot, :size, :]
                    up_a = jnp.dot(x, up[k, 0], preferred_element_type=F32)
                    up_b = jnp.dot(x, up[k, 1], preferred_element_type=F32)
                    hid[:size, k * up_cols:(k + 1) * up_cols] = (jax.nn.silu(up_a) * up_b).astype(BF16)

                sized(up_part)

                @pl.when(more)
                def _(k=k):
                    up_copy(i + 1, k, 0).start()
                    up_copy(i + 1, k, 1).start()

            for k in range(n_down):
                down_copy(i, k).wait()

                def down_part(size, k=k):
                    out = jnp.dot(hid[:size, :], down[k], preferred_element_type=F32).astype(BF16).astype(F32)
                    for g in range(down_groups):
                        row_scr[pl.ds(k * down_groups + g, size, stride=groups), :] = out[:, g * LANES:(g + 1) * LANES]

                sized(down_part)

                @pl.when(more)
                def _(k=k):
                    down_copy(i + 1, k).start()

            def add_rows(q, inner):
                ats, new = [], []
                for u in range(batch):
                    s = base + q * batch + u
                    at = pl.ds(tok_ref[s] * groups, groups)
                    ats.append(at)
                    new.append(acc[at, :] + gate_ref[s] * row_scr[pl.ds((q * batch + u) * groups, groups), :])
                for at, value in zip(ats, new):
                    acc[at, :] = value
                return inner

            lax.fori_loop(0, (count + batch - 1) // batch, add_rows, 0)
            return carry

        lax.fori_loop(0, n_items, item, 0)

    hbm = pl.BlockSpec(memory_space=pl.ANY)
    dma = pltpu.SemaphoreType.DMA
    return pl.pallas_call(
        kernel,
        out_shape=pltpu.VMEM((acc_rows, LANES), F32),
        grid_spec=pltpu.PrefetchScalarGridSpec(
            num_scalar_prefetch=3, grid=(), in_specs=[hbm] * 4, out_specs=pl.BlockSpec(memory_space=pltpu.VMEM),
            scratch_shapes=[
                pltpu.VMEM((ROW_TILE * groups, LANES), F32),
                pltpu.VMEM((ROW_TILE, ff), BF16), pltpu.VMEM((2, ROW_TILE, width), BF16),
                pltpu.VMEM((n_up, 2, width, up_cols), BF16), pltpu.VMEM((n_down, ff, down_cols), BF16),
                pltpu.SMEM((max_items,), I32), pltpu.SMEM((max_items,), I32), pltpu.SMEM((max_items,), I32),
                dma((2,)), dma((n_up, 2)), dma((n_down,))]),
        compiler_params=pltpu.CompilerParams(vmem_limit_bytes=34 * 1024 * 1024),
        cost_estimate=pl.CostEstimate(flops=6 * capacity * width * ff, bytes_accessed=6 * local_experts * width * ff, transcendentals=capacity * ff),
        name='experts',
    )(spans, slot_tok, slot_gate, rows_in, expert_w1, expert_w3, expert_w2)


def reduce_and_finish(sums, resid_in, normed, shared_w1, shared_w3, shared_w2, ep_size):
    chips = ep_size // 2
    tok_local, width = resid_in.shape
    ff = shared_w1.shape[1]
    groups = width // LANES
    pieces = 4
    tok_piece = tok_local // pieces
    piece_rows = tok_piece * groups
    up_cols = 256
    n_up = ff // up_cols
    down_cols = 256
    n_down = width // down_cols
    add_step = 128

    def kernel(sums_ref, resid_ref, x_ref, w1_ref, w3_ref, w2_ref, out_ref,
               pair, opp, home, up_buf, down_buf, hid, shared,
               pair_send, pair_recv, fwd_send, fwd_recv, bwd_send, bwd_recv, up_sem, down_sem):
        me = lax.axis_index('ep')
        chip, core = me // 2, lax.rem(me, 2)
        sibling = 2 * chip + 1 - core
        after = 2 * lax.rem(chip + 1, chips) + core
        before = 2 * lax.rem(chip + chips - 1, chips) + core

        def up_copy(j, slot, which):
            src = w1_ref if which == 0 else w3_ref
            return pltpu.make_async_copy(src.at[:, pl.ds(pl.multiple_of(j * up_cols, LANES), up_cols)], up_buf.at[slot, which], up_sem.at[slot, which])

        def down_copy(j, slot):
            return pltpu.make_async_copy(w2_ref.at[:, pl.ds(pl.multiple_of(j * down_cols, LANES), down_cols)], down_buf.at[slot], down_sem.at[slot])

        barrier = pltpu.get_barrier_semaphore()
        for peer in (sibling, after, before):
            pl.semaphore_signal(barrier, inc=1, device_id={'ep': peer}, device_id_type=pl.DeviceIdType.MESH)
        pl.semaphore_wait(barrier, 3)

        def block_piece(b, q):
            return sums_ref.at[pl.ds((b * pieces + q) * piece_rows, piece_rows), :]

        def to_pair(o, q):
            return pltpu.make_async_remote_copy(
                src_ref=block_piece(chips + o, q), dst_ref=pair.at[o, q], send_sem=pair_send.at[o, q], recv_sem=pair_recv.at[o, q],
                device_id={'ep': sibling}, device_id_type=pl.DeviceIdType.MESH)

        def ring(src, dst, send, recv, i, peer):
            return pltpu.make_async_remote_copy(
                src_ref=src, dst_ref=dst, send_sem=send.at[i], recv_sem=recv.at[i],
                device_id={'ep': peer}, device_id_type=pl.DeviceIdType.MESH)

        order = [(o, q) for o in (3, 2, 1, 0) for q in ((0, 2, 1, 3) if o == 3 else (2, 3, 0, 1) if o == 2 else (0, 1, 2, 3))]
        for o, q in order:
            to_pair(o, q).start()
        for slot in range(2):
            for which in range(2):
                up_copy(slot, slot, which).start()

        def add(o, q, src):
            def step(i, carry):
                at = pl.ds(pl.multiple_of(i * add_step, add_step), add_step)
                pair[o, q, at, :] = pair[o, q, at, :] + src[at, :]
                return carry

            lax.fori_loop(0, piece_rows // add_step, step, 0)

        def pair_sum(o, q):
            to_pair(o, q).wait_recv()
            add(o, q, block_piece(o, q))

        opp_fwd = [ring(pair.at[3, q], opp.at[q], fwd_send, fwd_recv, q, after) for q in (0, 1)]
        opp_bwd = [ring(pair.at[3, 2 + q], opp.at[2 + q], bwd_send, bwd_recv, q, before) for q in (0, 1)]
        home_fwd = {q: ring(pair.at[2, q], home.at[0, q], fwd_send, fwd_recv, 2 + q, after) for q in range(pieces)}
        home_bwd = {q: ring(pair.at[1, q], home.at[1, q], bwd_send, bwd_recv, 2 + q, before) for q in range(pieces)}
        for q in (0, 1):
            pair_sum(3, q)
            pair_sum(3, 2 + q)
            opp_fwd[q].start()
            opp_bwd[q].start()
        for q in (0, 1):
            pair_sum(2, 2 + q)
            pair_sum(1, q)
            home_fwd[2 + q].start()
            home_bwd[q].start()
        for q in (0, 1):
            pair_sum(2, q)
            pair_sum(1, 2 + q)

        def up_step(j, carry):
            slot = lax.rem(j, 2)
            up_copy(j, slot, 0).wait()
            up_copy(j, slot, 1).wait()
            up_a = jnp.dot(x_ref[...], up_buf[slot, 0], preferred_element_type=F32)
            up_b = jnp.dot(x_ref[...], up_buf[slot, 1], preferred_element_type=F32)
            hid[:, pl.ds(pl.multiple_of(j * up_cols, LANES), up_cols)] = (jax.nn.silu(up_a) * up_b).astype(BF16)

            @pl.when(j + 2 < n_up)
            def _():
                up_copy(j + 2, slot, 0).start()
                up_copy(j + 2, slot, 1).start()

            return carry

        for slot in range(2):
            down_copy(slot, slot).start()
        lax.fori_loop(0, n_up, up_step, 0)

        def down_step(j, carry):
            slot = lax.rem(j, 2)
            down_copy(j, slot).wait()
            part = jnp.dot(hid[...], down_buf[slot], preferred_element_type=F32)
            shared[:, pl.ds(pl.multiple_of(j * down_cols, LANES), down_cols)] = part.astype(BF16)

            @pl.when(j + 2 < n_down)
            def _():
                down_copy(j + 2, slot).start()

            return carry

        lax.fori_loop(0, n_down, down_step, 0)

        for q in range(pieces):
            pair_sum(0, q)
        for q in (0, 1):
            opp_fwd[q].wait_recv()
            add(2, q, opp.at[q])
            home_fwd[q].start()
            opp_bwd[q].wait_recv()
            add(1, 2 + q, opp.at[2 + q])
            home_bwd[2 + q].start()
        for q in (0, 1):
            home_fwd[2 + q].wait_recv()
            add(0, 2 + q, home.at[0, 2 + q])
            home_bwd[q].wait_recv()
            add(0, q, home.at[1, q])
        for q in (0, 2, 1, 3):
            way, late = (0, home_fwd[q]) if q < 2 else (1, home_bwd[q])
            late.wait_recv()
            rows = slice(q * tok_piece, (q + 1) * tok_piece)
            for g in range(groups):
                col = g * LANES
                at = pl.ds(g, tok_piece, stride=groups)
                routed = pair[0, q, at, :] + home[way, q, at, :]
                total = resid_ref[rows, col:col + LANES].astype(F32) + shared[rows, col:col + LANES].astype(F32) + routed
                out_ref[rows, col:col + LANES] = total.astype(BF16)
        for o, q in order:
            to_pair(o, q).wait_send()
        for copy in opp_fwd + opp_bwd + list(home_fwd.values()) + list(home_bwd.values()):
            copy.wait_send()

    hbm = pl.BlockSpec(memory_space=pl.ANY)
    vmem = pl.BlockSpec(memory_space=pltpu.VMEM)
    dma = pltpu.SemaphoreType.DMA
    return pl.pallas_call(
        kernel,
        out_shape=pltpu.VMEM((tok_local, width), BF16),
        in_specs=[vmem, vmem, vmem, hbm, hbm, hbm],
        out_specs=vmem,
        scratch_shapes=[
            pltpu.VMEM((chips, pieces, piece_rows, LANES), F32),
            pltpu.VMEM((pieces, piece_rows, LANES), F32), pltpu.VMEM((2, pieces, piece_rows, LANES), F32),
            pltpu.VMEM((2, 2, width, up_cols), BF16), pltpu.VMEM((2, ff, down_cols), BF16),
            pltpu.VMEM((tok_local, ff), BF16), pltpu.VMEM((tok_local, width), BF16),
            dma((chips, pieces)), dma((chips, pieces)), dma((6,)), dma((6,)), dma((6,)), dma((6,)), dma((2, 2)), dma((2,))],
        compiler_params=pltpu.CompilerParams(collective_id=1, has_side_effects=True, vmem_limit_bytes=37 * 1024 * 1024),
        cost_estimate=pl.CostEstimate(flops=6 * tok_local * width * ff, bytes_accessed=6 * width * ff, transcendentals=tok_local * ff),
        name='reduce_and_finish',
    )(pltpu.with_memory_space_constraint(sums, pltpu.VMEM), resid_in, normed, shared_w1, shared_w3, shared_w2)


def solution(mesh):
    ep_size = mesh.shape['ep']
    tok_spec = P(('dp', 'ep'))
    expert_spec = P('ep')

    def device_fn(resid_in, expert_ids, priority, norm_gain, router_w, shared_w1, shared_w3, shared_w2, expert_w1, expert_w3, expert_w2):
        tok_local, width = resid_in.shape
        top_k = expert_ids.shape[1]
        local_experts = expert_w1.shape[0]
        capacity = tok_local * top_k
        n_tokens = tok_local * ep_size
        slots = -(-(capacity + local_experts * ALIGN + ROW_TILE) // LANES) * LANES
        normed, meta = norm_and_gates(resid_in, norm_gain, router_w.T, expert_ids.T, priority.T)
        rows_in, slot_tok, slot_gate, spans = dispatch(meta, normed, local_experts, capacity, slots, ep_size)
        spans = spans.reshape(-1)
        sums = experts(spans, slot_tok.reshape(-1), slot_gate.reshape(-1), rows_in, expert_w1, expert_w3, expert_w2, n_tokens, capacity)
        return reduce_and_finish(sums, resid_in, normed, shared_w1, shared_w3, shared_w2, ep_size)

    return jax.shard_map(device_fn, mesh=mesh, in_specs=(tok_spec, tok_spec, tok_spec, P(), P(), P(), P(), P(), expert_spec, expert_spec, expert_spec), out_specs=tok_spec, check_vma=False)
```
